32 devices in a mesh: dp: 8 (over z, x), row: 2 (over core), col: 2 (over y).
Axes of the slice: x: 2, y: 2, z: 4, core: 2. Of those that a mesh axis runs over, the one named last changes fastest.
Arguments:
- tokens: bfloat16 [8, 2048, 768], P('dp', 'col', 'row'), may hold values from -7 to 7
- cotangent: bfloat16 [8, 2048, 768], P('dp', 'col', 'row'), may hold values from -6 to 6
- segments: int32 [8, 2048], P('dp', 'row'), may hold values from 0 to 3, never falling along the last dimension, each value on 1 to 1024 neighbouring positions
- valid: int32 [8, 2048], P('dp', 'col'), may hold values 0 or 1
- w_query: bfloat16 [2, 768, 768], P(None, 'row', 'col'), may hold values from -0.21875 to 0.21875
- w_key: bfloat16 [2, 768, 768], P(None, 'row', 'col'), may hold values from -0.21875 to 0.21875
- w_value: bfloat16 [2, 768, 768], P(None, 'row', 'col'), may hold values from -0.21875 to 0.21875
- w_out: bfloat16 [2, 768, 768], P(None, 'col', 'row'), may hold values from -3.5 to 3.5
- w_up: bfloat16 [2, 768, 3072], P(None, 'row', 'col'), may hold values from -0.21875 to 0.21875
- w_down: bfloat16 [2, 3072, 768], P(None, 'col', 'row'), may hold values from -0.109375 to 0.109375
- vectors: float32 [2, 9216], replicated, may hold values from -2 to 2, as said below
- vector_m: float32 [2, 9216], replicated, may hold values from -224 to 224
- vector_v: float32 [2, 9216], replicated, may hold values from 163.84 to 16384
- tile_order: int32 [2, 2, 216], P('row', 'col'), may hold values from 0 to 215, each once within a row
- basis_left: float32 [2, 2, 216, 128, 128], P('row', 'col', 'dp'), may hold values from -0.5 to 0.5
- basis_right: float32 [2, 2, 216, 128, 128], P('row', 'col', 'dp'), may hold values from -0.5 to 0.5
- tile_m: float32 [2, 2, 216, 128, 128], P('row', 'col', 'dp'), may hold values from -224 to 224
- tile_v: float32 [2, 2, 216, 128, 128], P('row', 'col', 'dp'), may hold values from 163.84 to 16384
Outputs:
- final_out: bfloat16 [8, 2048, 768], P('dp', 'col', 'row')
- grad_tokens: float32 [8, 2048, 768], P('dp', 'col', 'row')
- statistics: float32 [2], replicated
- vector_grad: float32 [2, 9216], replicated
- vector_m_new: float32 [2, 9216], replicated
- vector_v_new: float32 [2, 9216], replicated
- vector_update: float32 [2, 9216], replicated
- tile_grad: float32 [2, 2, 216, 128, 128], P('row', 'col', 'dp')
- tile_m_new: float32 [2, 2, 216, 128, 128], P('row', 'col', 'dp')
- tile_v_new: float32 [2, 2, 216, 128, 128], P('row', 'col', 'dp')
- tile_update: float32 [2, 2, 216, 128, 128], P('row', 'col', 'dp')
The draws below stay inside these ranges and needn't reach their ends.
Inputs may be any that keep to these rules, and one draw needn't show every extreme that they name: `segments`: each sequence's ids start at 0 and rise by one from document to document. `tile_order`: each row (r, c) names every code once, so every owner takes at most 27 tiles and owner 0 takes 27. `vectors`: gains lie in 0.1 to 1.9.
All inputs are finite; a program needn't handle non-finite values. No bound on the sum of `valid` on one device may be relied on, other than what follows from the above.
Results may differ from the reference program's by a relative error of at most 0.022.
Values may be sent and summed in bfloat16 or wider, within the bound.
A program may use at most 384 MiB of HBM per device.

```python
import math
import jax
import jax.numpy as jnp
import numpy as np
from jax import lax

D = 768
H = 12
DH = 64
FF = 3072
LAYERS = 2
HALF = 512
QBLK = 512
TILE = 128
SEQ_LEN = 2048
NSEQ = 8
TOKENS = 16384
VEC = 9216
NT = 216
CAP = 27
N_DP = 8
N_ROW = 2
N_COL = 2


def draw_tokens(key, part):
    shape = (NSEQ, SEQ_LEN, D)
    seq_frac = jnp.arange(NSEQ).astype(jnp.float32) / max(NSEQ - 1, 1)
    base = jnp.clip(jax.random.normal(key, shape, jnp.float32), -4.0, 4.0)
    ramp = jnp.exp(0.5 * math.log(3.0) * seq_frac)
    return (base * ramp[:, None, None]).astype(jnp.bfloat16)


def draw_vectors(key, part):
    shape = (LAYERS, 8 * D + FF)
    noise = jax.random.normal(key, shape, jnp.float32)
    column = jnp.arange(8 * D + FF)
    is_gain = (column >= 4 * D) & (column < 5 * D) | (column >= 6 * D) & (column < 7 * D)
    gains = 1.0 + 0.3 * jnp.clip(noise, -3.0, 3.0)
    biases = 0.5 * jnp.clip(noise, -4.0, 4.0)
    return jnp.where(is_gain[None, :], gains, biases)


def plant(result, stream_key, least, largest):
    shape = result.shape
    spot = [jax.random.randint(jax.random.fold_in(stream_key, axis), (), 0, shape[axis]) for axis in range(len(shape))]
    result = result.at[tuple(spot)].set(least)
    longest = shape.index(max(shape))
    spot[longest] = (spot[longest] + 1) % shape[longest]
    return result.at[tuple(spot)].set(largest)


def block_levels(stream_key, shape, cuts, least, top_value):
    def one(axis_at, shards_of):
        draws = jax.random.uniform(jax.random.fold_in(jax.random.fold_in(stream_key, 6), axis_at), (shards_of,), jnp.float32, least / len(cuts), top_value / len(cuts))
        return jnp.repeat(jnp.exp(draws), shape[axis_at] // shards_of).reshape((-1,) + (1,) * (len(shape) - axis_at - 1))

    loudness = one(*cuts[0])
    for cut in cuts[1:]:
        loudness = loudness * one(*cut)
    return loudness


def length_profile(number_of, total, reach, skew):
    portions = [(1 << 20) // math.isqrt(rank ** skew) + 1 for rank in range(2, number_of + 1)]
    spare, holding = total - reach - (number_of - 1), [1] * (number_of - 1)
    while spare > 0:
        candidates = [i for i in range(number_of - 1) if holding[i] < reach]
        mass, budget = sum([portions[i] for i in candidates]), spare
        for i in candidates:
            addition = min(reach - holding[i], max(1, budget * portions[i] // mass), spare)
            holding[i] = holding[i] + addition
            spare = spare - addition
    return np.array([reach] + holding)


def uneven(stream_key, amount, total, reach, slope):
    if amount == 2:
        one = jax.random.randint(stream_key, (), max(1, total - reach), min(reach, total - 1) + 1)
        return jnp.stack([one, total - one])
    lengths = jnp.asarray(length_profile(amount, total, reach, slope), jnp.int32)
    couples = (amount - 1) // 2
    giver, receiver = lengths[1:1 + 2 * couples:2], lengths[2:2 + 2 * couples:2]
    room = jnp.minimum(giver - 1, reach - receiver)
    moved = jax.random.randint(jax.random.fold_in(stream_key, 1), (couples,), 0, 1 << 20) % (room + 1)
    lengths = lengths.at[1:1 + 2 * couples:2].set(giver - moved).at[2:2 + 2 * couples:2].set(receiver + moved)
    return lengths[jax.random.permutation(jax.random.fold_in(stream_key, 2), amount)]


def scatter_about(own_key, dims, spread, limit, split=(), dtype=jnp.bfloat16):
    array = jax.random.normal(own_key, dims, jnp.float32) * spread
    if len(split) > 0:
        array = block_levels(own_key, dims, split, -0.22, 0.18) * array
    return jnp.clip(array, min=-limit, max=limit).astype(dtype)


def setup_inputs(seed: int = 0) -> dict:
    key_of = jax.random.split(jax.random.key(seed), 19)
    return {
        "tokens": draw_tokens(jax.random.fold_in(key_of[18], 71), 0),
        "cotangent": scatter_about(key_of[1], (NSEQ, SEQ_LEN, D), 1.0, 6.0, ((0, 8), (1, 2), (2, 2))),
        "segments": jax.vmap(lambda own: jnp.searchsorted(jnp.cumsum(uneven(own, 4, SEQ_LEN, SEQ_LEN // 2, 0)), jnp.arange(SEQ_LEN), side="right"))(jax.random.split(key_of[2], NSEQ)).reshape((NSEQ, SEQ_LEN)).astype(jnp.int32),
        "valid": plant((jax.random.randint(key_of[3], (NSEQ, SEQ_LEN), 0, 16) < 15).astype(jnp.int32), jax.random.fold_in(key_of[3], 1), 0, 1),
        "w_query": scatter_about(key_of[4], (LAYERS, D, D), D ** -0.5, 0.21875, ((1, 2), (2, 2))),
        "w_key": scatter_about(key_of[5], (LAYERS, D, D), D ** -0.5, 0.21875, ((1, 2), (2, 2))),
        "w_value": scatter_about(key_of[6], (LAYERS, D, D), D ** -0.5, 0.21875, ((1, 2), (2, 2))),
        "w_out": scatter_about(key_of[7], (LAYERS, D, D), (max(2 * D // HALF, 1)) ** -0.5, 3.5, ((1, 2), (2, 2))),
        "w_up": scatter_about(key_of[8], (LAYERS, D, FF), D ** -0.5, 0.21875, ((1, 2), (2, 2))),
        "w_down": scatter_about(key_of[9], (LAYERS, FF, D), FF ** -0.5, 0.109375, ((1, 2), (2, 2))),
        "vectors": draw_vectors(jax.random.fold_in(key_of[18], 71), 0),
        "vector_m": scatter_about(key_of[11], (LAYERS, VEC), (0.3 * TOKENS ** 0.5), 224.0, (), jnp.float32),
        "vector_v": jnp.clip(jnp.exp(jax.random.uniform(key_of[12], (LAYERS, VEC), jnp.float32, math.log(163.84), math.log(16384.0))), 163.84, 16384.0),
        "tile_order": jax.vmap(lambda own: jax.random.permutation(own, NT))(jax.random.split(key_of[13], N_ROW * N_COL)).reshape((N_ROW, N_COL, NT)).astype(jnp.int32),
        "basis_left": scatter_about(key_of[14], (N_ROW, N_COL, N_DP * CAP, TILE, TILE), TILE ** -0.5, 0.5, ((0, 2), (1, 2), (2, 8)), jnp.float32),
        "basis_right": scatter_about(key_of[15], (N_ROW, N_COL, N_DP * CAP, TILE, TILE), TILE ** -0.5, 0.5, ((0, 2), (1, 2), (2, 8)), jnp.float32),
        "tile_m": scatter_about(key_of[16], (N_ROW, N_COL, N_DP * CAP, TILE, TILE), (0.3 * TOKENS ** 0.5), 224.0, ((0, 2), (1, 2), (2, 8)), jnp.float32),
        "tile_v": jnp.clip(jnp.exp(math.log(16384.0) - 4.6051702 * jax.random.uniform(key_of[17], (N_ROW, N_COL, N_DP * CAP, TILE, TILE), jnp.float32) ** block_levels(key_of[17], (N_ROW, N_COL, N_DP * CAP, TILE, TILE), ((0, 2), (1, 2), (2, 8)), -0.2, 0.2)), 163.84, 16384.0),
    }


@jax.custom_vjp
def low(v):
    return lax.optimization_barrier(v.astype(jnp.bfloat16)).astype(jnp.float32)

@jax.custom_vjp
def low_back(v):
    return v

def low_keep(v):
    return (low(v), None)

def low_pass(kept, grad):
    return (grad,)

def back_keep(v):
    return (v, None)

def back_low(kept, grad):
    return (low(grad),)
low.defvjp(low_keep, low_pass)
low_back.defvjp(back_keep, back_low)
HIGHEST = lax.Precision.HIGHEST
NEG_BIG = -1e+30
NORM_EPS = 1e-06
ADAM_EPS = 1e-08
TILE_RATE = 0.03
VECTOR_RATE = 0.1
DECAY = 0.5

def product(left_mat, right_mat):
    return jnp.dot(left_mat, right_mat, precision=HIGHEST)

def layer_norm(resid, gain_vec, shift_vec):
    row_mean = lax.optimization_barrier(jnp.mean(resid, axis=-1, keepdims=True))
    centred = resid - row_mean
    row_var = lax.optimization_barrier(jnp.mean(centred * centred, axis=-1, keepdims=True))
    return centred * lax.rsqrt(row_var + NORM_EPS) * gain_vec + shift_vec

def attend_sequence(operands):
    queries, key_rows, value_rows, seg_ids = operands
    key_heads = key_rows.reshape(SEQ_LEN, H, DH)
    value_heads = value_rows.reshape(SEQ_LEN, H, DH)
    key_pos = jnp.arange(SEQ_LEN).astype(jnp.int32)

    def one_block(offset):
        query_heads = lax.dynamic_slice_in_dim(queries, offset, QBLK, 0).reshape(QBLK, H, DH)
        raw_scores = jnp.einsum('qhd,khd->hqk', query_heads, key_heads, precision=HIGHEST) * DH ** (-0.5)
        raw_scores = low_back(raw_scores)
        query_pos = offset + jnp.arange(QBLK).astype(jnp.int32)
        query_seg = lax.dynamic_slice_in_dim(seg_ids, offset, QBLK, 0)
        visible = (query_seg[:, None] == seg_ids[None, :]) & (jnp.abs(query_pos[:, None] - key_pos[None, :]) < HALF)
        raw_scores = jnp.where(visible[None], raw_scores, NEG_BIG)
        softmax_w = low(jax.nn.softmax(raw_scores, axis=-1))
        return jnp.einsum('hqk,khd->qhd', softmax_w, value_heads, precision=HIGHEST).reshape(QBLK, H * DH)
    offsets = (jnp.arange(SEQ_LEN // QBLK) * QBLK).astype(jnp.int32)
    return lax.map(jax.checkpoint(one_block), offsets).reshape(SEQ_LEN, H * DH)

def vector_parts(vec_row):
    return tuple((vec_row[spot * D:(spot + 1) * D] for spot in range(8))) + (vec_row[8 * D:8 * D + FF],)

def block_layer(hidden, weights, vec_row, segments):
    w_query, w_key, w_value, w_out, w_up, w_down = weights
    bias_q, bias_v, bias_o, bias_down, gain_one, shift_one, gain_two, shift_two, bias_up = vector_parts(vec_row)
    inputs = low(hidden)
    queries = low_back(low(product(inputs, w_query) + bias_q))
    key_rows = low_back(low(product(inputs, w_key)))
    value_rows = low_back(low(product(inputs, w_value) + bias_v))
    seq_shape = (NSEQ, SEQ_LEN, H * DH)
    attended = lax.map(jax.checkpoint(attend_sequence), (queries.reshape(seq_shape), key_rows.reshape(seq_shape), value_rows.reshape(seq_shape), segments))
    attended = low_back(low(attended.reshape(TOKENS, H * DH)))
    branch = low_back(product(attended, w_out) + bias_o)
    resid_one = hidden + branch
    normed_out = layer_norm(resid_one, gain_one, shift_one)
    mid_bf = low(normed_out)
    up_proj = low_back(product(mid_bf, w_up) + bias_up)
    activated = low(jax.nn.gelu(up_proj, approximate=False))
    down_proj = low_back(product(activated, w_down) + bias_down)
    return (layer_norm(normed_out + down_proj, gain_two, shift_two), resid_one, branch)

def network(tokens, w_query, w_key, w_value, w_out, w_up, w_down, vectors, segments):
    hidden = tokens.reshape(TOKENS, D)
    first_stats = None
    for layer_pos in range(LAYERS):
        weights = (w_query[layer_pos], w_key[layer_pos], w_value[layer_pos], w_out[layer_pos], w_up[layer_pos], w_down[layer_pos])
        hidden, resid_one, branch = block_layer(hidden, weights, vectors[layer_pos], segments)
        if layer_pos == 0:
            first_stats = (resid_one, branch)
    return (hidden, first_stats)

def block_tiles(block_mat):
    row_span, col_span = block_mat.shape
    return block_mat.reshape(row_span // TILE, TILE, col_span // TILE, TILE).transpose(0, 2, 1, 3).reshape(-1, TILE, TILE)

def owner_slots(grad_mats, tile_order):
    groups = []
    for row_pos in range(N_ROW):
        for col_pos in range(N_COL):
            pieces = []
            for layer_pos in range(LAYERS):
                for mat_pos in range(6):
                    full_mat = grad_mats[mat_pos][layer_pos]
                    if mat_pos in (0, 1, 2, 4):
                        row_size = full_mat.shape[0] // N_ROW
                        col_size = full_mat.shape[1] // N_COL
                        block_mat = full_mat[row_pos * row_size:(row_pos + 1) * row_size, col_pos * col_size:(col_pos + 1) * col_size]
                    else:
                        row_size = full_mat.shape[0] // N_COL
                        col_size = full_mat.shape[1] // N_ROW
                        block_mat = full_mat[col_pos * row_size:(col_pos + 1) * row_size, row_pos * col_size:(row_pos + 1) * col_size]
                    pieces.append(block_tiles(block_mat))
            tile_list = jnp.concatenate(pieces, 0)
            owner_row = tile_order[row_pos, col_pos]
            targets = owner_row % N_DP * CAP + owner_row // N_DP
            outbox = jnp.zeros((N_DP * CAP, TILE, TILE), jnp.float32).at[targets].set(tile_list)
            groups.append(outbox)
    return jnp.stack(groups, 0).reshape(N_ROW, N_COL, N_DP * CAP, TILE, TILE)

def rotate_update(grad_tiles, left_basis, right_basis, old_m, old_v):
    turned = jnp.einsum('...ji,...jk->...ik', left_basis, grad_tiles, precision=HIGHEST)
    rotated = jnp.einsum('...ik,...kl->...il', turned, right_basis, precision=HIGHEST)
    new_m = DECAY * old_m + (1.0 - DECAY) * rotated
    new_v = DECAY * old_v + (1.0 - DECAY) * rotated * rotated
    direction = new_m / (jnp.sqrt(new_v) + ADAM_EPS)
    back_turn = jnp.einsum('...ij,...jk->...ik', left_basis, direction, precision=HIGHEST)
    update = -TILE_RATE * jnp.einsum('...ik,...lk->...il', back_turn, right_basis, precision=HIGHEST)
    return (new_m, new_v, update)

def reference(tokens, cotangent, segments, valid, w_query, w_key, w_value, w_out, w_up, w_down, vectors, vector_m, vector_v, tile_order, basis_left, basis_right, tile_m, tile_v):
    floats = [arr.astype(jnp.float32) for arr in (tokens, w_query, w_key, w_value, w_out, w_up, w_down)]

    def closed(tok_in, wq_in, wk_in, wv_in, wo_in, wu_in, wd_in, vec_in):
        return network(tok_in, wq_in, wk_in, wv_in, wo_in, wu_in, wd_in, vec_in, segments)
    final_hidden, pullback, first_stats = jax.vjp(closed, *floats, vectors, has_aux=True)
    mask_rows = valid.astype(jnp.float32).reshape(TOKENS)
    seed_grad = cotangent.astype(jnp.float32).reshape(TOKENS, D) * mask_rows[:, None]
    grads = pullback(seed_grad)
    grad_tokens = grads[0].reshape(NSEQ, SEQ_LEN, D)
    resid_one, branch = first_stats
    valid_count = jnp.sum(mask_rows)
    resid_total = jnp.sum(mask_rows * lax.optimization_barrier(jnp.sum(resid_one * resid_one, axis=1)))
    branch_total = jnp.sum(mask_rows * lax.optimization_barrier(jnp.sum(branch * branch, axis=1)))
    statistics = jnp.sqrt(jnp.stack((resid_total, branch_total)) / (D * valid_count))
    vector_grad = grads[7]
    vector_m_new = DECAY * vector_m + (1.0 - DECAY) * vector_grad
    vector_v_new = DECAY * vector_v + (1.0 - DECAY) * vector_grad * vector_grad
    vector_update = -VECTOR_RATE * vector_m_new / (jnp.sqrt(vector_v_new) + ADAM_EPS)
    tile_grad = owner_slots(grads[1:7], tile_order)
    tile_m_new, tile_v_new, tile_update = rotate_update(tile_grad, basis_left, basis_right, tile_m, tile_v)
    final_out = final_hidden.reshape(NSEQ, SEQ_LEN, D).astype(jnp.bfloat16)
    return (final_out, grad_tokens, statistics, vector_grad, vector_m_new, vector_v_new, vector_update, tile_grad, tile_m_new, tile_v_new, tile_update)
```

```python
import functools

import jax
import jax.numpy as jnp
from jax import lax
from jax.experimental import pallas as pl
from jax.experimental.pallas import tpu as pltpu
from jax.sharding import PartitionSpec as P

D = 768
DH = 64
LAYERS = 2
HALF = 512
TILE = 128
HF = 384
FFC = 1536
FT = 512
STEPS = FFC // FT
TOK = 512
QB = 128
KSPAN = QB + 2 * HALF
PAIRS = 6

HIGHEST = lax.Precision.HIGHEST
NEG_BIG = -1e30
NORM_EPS = 1e-06
ADAM_EPS = 1e-08
TILE_RATE = 0.03
VECTOR_RATE = 0.1
DECAY = 0.5
F32 = jnp.float32
BF16 = jnp.bfloat16
SWAP = ((0, 1), (1, 0))


def dot(a, b):
    return lax.dot_general(a, b, (((1,), (0,)), ((), ())), preferred_element_type=F32)


def dot_bt(a, b):
    return lax.dot_general(a, b, (((1,), (1,)), ((), ())), preferred_element_type=F32)


def dot_at(a, b):
    return lax.dot_general(a, b, (((0,), (0,)), ((), ())), preferred_element_type=F32)


def sds(shape, dtype):
    return jax.ShapeDtypeStruct(shape, dtype)


def whole(shape):
    return pl.BlockSpec(shape, lambda *_: (0,) * len(shape))


SMEM_SPEC = pl.BlockSpec(memory_space=pltpu.SMEM)


def cost(flops, nbytes):
    return pl.CostEstimate(flops=int(flops), bytes_accessed=int(nbytes), transcendentals=0)


def params():
    return pltpu.CompilerParams(vmem_limit_bytes=60 * 1024 * 1024)


def qkv_kernel(rc, x_ref, w00, w01, w10, w11, vec, q_ref, kv_ref):
    for rel_c, (w_near, w_far) in enumerate(((w00, w10), (w01, w11))):
        c = rc[1] ^ rel_c
        acc = dot(x_ref[0], w_near[...]) + dot(x_ref[1], w_far[...])
        q = (acc[:, :HF] + vec[c]).astype(BF16)
        q_ref[c] = (q.astype(F32) * DH ** (-0.5)).astype(BF16)
        kv_ref[c, 0] = acc[:, HF : 2 * HF].astype(BF16)
        kv_ref[c, 1] = (acc[:, 2 * HF :] + vec[2 + c]).astype(BF16)


def qkv_forward(rc, x, pieces, va):
    rows = 256
    return pl.pallas_call(
        qkv_kernel,
        grid=(TOK // rows,),
        in_specs=[SMEM_SPEC, pl.BlockSpec((2, rows, HF), lambda i: (0, i, 0))]
        + [whole((HF, 3 * HF))] * 4
        + [whole((16, 1, HF))],
        out_specs=[
            pl.BlockSpec((2, rows, HF), lambda i: (0, i, 0)),
            pl.BlockSpec((2, 2, rows, HF), lambda i: (0, 0, i, 0)),
        ],
        out_shape=[sds((2, TOK, HF), BF16), sds((2, 2, TOK, HF), BF16)],
        compiler_params=params(),
        cost_estimate=cost(2 * TOK * D * 3 * D, 7e6),
        name="qkv",
    )(rc, x, *pieces, va)


def fill_bias(bias, segk_ref, segq_ref, b):
    off = pl.multiple_of(b * QB, QB)
    seg_k = segk_ref[pl.ds(off, KSPAN), :]
    key = lax.broadcasted_iota(jnp.int32, (KSPAN, QB), 0)
    query = lax.broadcasted_iota(jnp.int32, (KSPAN, QB), 1)
    seen = (seg_k == segq_ref[b]) & (jnp.abs(key - query - HALF) < HALF)
    bias[b] = jnp.where(seen, 0.0, NEG_BIG).astype(F32)


def fill_keys(ext, left, own, right):
    ext[0:TOK] = left[0, 0]
    ext[TOK : 2 * TOK] = own[0, 0]
    ext[2 * TOK :] = right[0, 0]


def split_pair(block):
    lane = lax.broadcasted_iota(jnp.int32, block.shape, 1)
    zero = jnp.zeros_like(block)
    return jnp.concatenate(
        (jnp.where(lane < DH, block, zero), jnp.where(lane >= DH, block, zero)), 0
    )


def join_pair(turned):
    return jnp.concatenate((turned[:DH, :QB], turned[DH:, QB:]), 0)


def attn_fwd_kernel(
    segk_ref, segq_ref, q_ref, kl, ko, kr, vl, vo, vr, o_ref, lse_ref, kext, vturn, bias
):
    h = pl.program_id(0)
    b = pl.program_id(1)

    @pl.when(b == 0)
    def _():
        fill_keys(kext, kl, ko, kr)
        for place, part in enumerate((vl, vo, vr)):
            vturn[:, place * TOK : (place + 1) * TOK] = part[0, 0].T

    @pl.when(h == 0)
    def _():
        fill_bias(bias, segk_ref, segq_ref, b)

    off = pl.multiple_of(b * QB, QB)
    qz = split_pair(q_ref[0])
    scores = dot_bt(kext[pl.ds(off, KSPAN), :], qz)
    extra = bias[b]
    scores = scores + jnp.concatenate((extra, extra), 1)
    top = jnp.max(scores, 0, keepdims=True)
    weights = jnp.exp(scores - top)
    total = jnp.sum(weights, 0, keepdims=True)
    turned = dot(vturn[:, pl.ds(off, KSPAN)], weights.astype(BF16)) / total
    o_ref[0] = join_pair(turned).T.astype(BF16)
    lse_ref[0, 0] = top + jnp.log(total)


def pair_specs():
    def kv_spec(which):
        return pl.BlockSpec((1, 1, TOK, TILE), lambda h, b: (h // 3, which, 0, h % 3))

    q_spec = pl.BlockSpec((1, QB, TILE), lambda h, b: (h // 3, b, h % 3))
    lse_spec = pl.BlockSpec((1, 1, 1, 2 * QB), lambda h, b: (h, b, 0, 0))
    return q_spec, kv_spec(0), kv_spec(1), lse_spec


def attn_forward(segk, segq, q, kv, left, right):
    q_spec, k_spec, v_spec, lse_spec = pair_specs()
    return pl.pallas_call(
        attn_fwd_kernel,
        grid=(PAIRS, TOK // QB),
        in_specs=[whole(segk.shape), whole(segq.shape), q_spec] + [k_spec] * 3 + [v_spec] * 3,
        out_specs=[q_spec, lse_spec],
        out_shape=[sds((2, TOK, HF), BF16), sds((PAIRS, TOK // QB, 1, 2 * QB), F32)],
        scratch_shapes=[
            pltpu.VMEM((3 * TOK, TILE), BF16),
            pltpu.VMEM((TILE, 3 * TOK), BF16),
            pltpu.VMEM((TOK // QB, KSPAN, QB), F32),
        ],
        compiler_params=params(),
        cost_estimate=cost(15e9, 8e6),
        name="attn_fwd",
    )(segk, segq, q, left, kv, right, left, kv, right)


def attn_bwd_kernel(
    segk_ref, segq_ref, q_ref, g_ref, lse_ref, kl, ko, kr, vl, vo, vr,
    dq_ref, dl_ref, do_ref, dr_ref, kext, vext, kturn, bias, dk, dv,
):
    h = pl.program_id(0)
    b = pl.program_id(1)

    @pl.when(b == 0)
    def _():
        fill_keys(kext, kl, ko, kr)
        fill_keys(vext, vl, vo, vr)
        for place, part in enumerate((kl, ko, kr)):
            kturn[:, place * TOK : (place + 1) * TOK] = part[0, 0].T
        dk[...] = jnp.zeros_like(dk)
        dv[...] = jnp.zeros_like(dv)

    @pl.when(h == 0)
    def _():
        fill_bias(bias, segk_ref, segq_ref, b)

    off = pl.multiple_of(b * QB, QB)
    span = pl.ds(off, KSPAN)
    qz = split_pair(q_ref[0])
    gz = split_pair(g_ref[0])
    scores = dot_bt(kext[span, :], qz)
    extra = bias[b]
    weights = jnp.exp(scores + jnp.concatenate((extra, extra), 1) - lse_ref[0, 0])
    d_weights = dot_bt(vext[span, :], gz)
    row_dot = jnp.sum(weights * d_weights, 0, keepdims=True)
    d_scores = (weights * (d_weights - row_dot)).astype(BF16)
    dv[span, :] += dot(weights.astype(BF16), gz)
    dk[span, :] += dot(d_scores, qz)
    turned = dot(kturn[:, span], d_scores)
    dq_ref[0] = (join_pair(turned).T * DH ** (-0.5)).astype(BF16)

    @pl.when(b == TOK // QB - 1)
    def _():
        for which, grads in enumerate((dk, dv)):
            dl_ref[0, which] = grads[0:TOK].astype(BF16)
            do_ref[0, which] = grads[TOK : 2 * TOK]
            dr_ref[0, which] = grads[2 * TOK :].astype(BF16)


def attn_backward(segk, segq, q, g, lse, kv, left, right):
    q_spec, k_spec, v_spec, lse_spec = pair_specs()
    d_spec = pl.BlockSpec((1, 2, TOK, TILE), lambda h, b: (h // 3, 0, 0, h % 3))
    d_shape = (2, 2, TOK, HF)
    return pl.pallas_call(
        attn_bwd_kernel,
        grid=(PAIRS, TOK // QB),
        in_specs=[whole(segk.shape), whole(segq.shape), q_spec, q_spec, lse_spec]
        + [k_spec] * 3
        + [v_spec] * 3,
        out_specs=[q_spec, d_spec, d_spec, d_spec],
        out_shape=[
            sds((2, TOK, HF), BF16), sds(d_shape, BF16), sds(d_shape, F32), sds(d_shape, BF16),
        ],
        scratch_shapes=[
            pltpu.VMEM((3 * TOK, TILE), BF16),
            pltpu.VMEM((3 * TOK, TILE), BF16),
            pltpu.VMEM((TILE, 3 * TOK), BF16),
            pltpu.VMEM((TOK // QB, KSPAN, QB), F32),
            pltpu.VMEM((3 * TOK, TILE), F32),
            pltpu.VMEM((3 * TOK, TILE), F32),
        ],
        compiler_params=params(),
        cost_estimate=cost(30e9, 16e6),
        name="attn_bwd",
    )(segk, segq, q, g, lse, left, kv, right, left, kv, right)


def feature_sum(near, far):
    return jnp.sum(near, 1, keepdims=True) + jnp.sum(far, 1, keepdims=True)


def norm_pair(near, far):
    mean = feature_sum(near, far) / D
    near = near - mean
    far = far - mean
    inv = lax.rsqrt(feature_sum(near * near, far * far) / D + NORM_EPS)
    return near * inv, far * inv, inv


def norm_pair_back(grads, normed, inv, gains):
    dn = [g * gain for g, gain in zip(grads, gains)]
    first = feature_sum(*dn) / D
    second = feature_sum(*[d * n for d, n in zip(dn, normed)]) / D
    return [inv * (d - first - n * second) for d, n in zip(dn, normed)]


def out_kernel(rc, a_ref, w00, w01, w10, w11, hid_ref, valid_ref, vec,
               norm_ref, mid_ref, n_ref, inv_ref, stat_ref):
    keep = valid_ref[...]
    resid = []
    sums = []
    for rel_r, (w_near, w_far) in enumerate(((w00, w01), (w10, w11))):
        r = rc[0] ^ rel_r
        branch = dot(a_ref[rc[1]], w_near[...]) + dot(a_ref[rc[1] ^ 1], w_far[...]) + vec[4 + r]
        total = hid_ref[rel_r].astype(F32) + branch
        resid.append(total)
        sums.append((total * total, branch * branch))

    @pl.when(pl.program_id(0) == 0)
    def _():
        stat_ref[...] = jnp.zeros_like(stat_ref)

    for which in range(2):
        part = (sums[0][which] + sums[1][which]) * keep
        stat_ref[which] += jnp.sum(part, 0, keepdims=True)
    near, far, inv = norm_pair(*resid)
    for rel_r, n in enumerate((near, far)):
        r = rc[0] ^ rel_r
        out = n * vec[8 + r] + vec[10 + r]
        norm_ref[rel_r] = out
        mid_ref[rel_r] = out.astype(BF16)
        n_ref[rel_r] = n
    inv_ref[...] = inv


def out_forward(rc, attended, pieces, hidden, valid, va):
    rows = 256
    half = pl.BlockSpec((2, rows, HF), lambda i: (0, i, 0))
    col = pl.BlockSpec((rows, 1), lambda i: (i, 0))
    return pl.pallas_call(
        out_kernel,
        grid=(TOK // rows,),
        in_specs=[SMEM_SPEC, half] + [whole((HF, HF))] * 4 + [half, col, whole((16, 1, HF))],
        out_specs=[half, half, half, col, whole((2, 1, HF))],
        out_shape=[
            sds((2, TOK, HF), F32), sds((2, TOK, HF), BF16), sds((2, TOK, HF), F32),
            sds((TOK, 1), F32), sds((2, 1, HF), F32),
        ],
        compiler_params=params(),
        cost_estimate=cost(2 * TOK * D * D, 7e6),
        name="attn_out",
    )(rc, attended, *pieces, hidden, valid, va)


def gelu_parts(u):
    bell = jnp.exp(-0.5 * u * u)
    t = 1.0 / (1.0 + (0.3275911 * 0.7071067811865476) * jnp.abs(u))
    poly = t * (0.5 * 0.254829592 + t * (0.5 * -0.284496736 + t * (
        0.5 * 1.421413741 + t * (0.5 * -1.453152027 + t * (0.5 * 1.061405429)))))
    tail = poly * bell
    below = jnp.where(u >= 0, 1.0 - tail, tail)
    return u * below, below + u * bell * 0.3989422804014327


def up_spec(rel_c):
    return pl.BlockSpec((HF, FT), lambda f: (0, jnp.clip(f - STEPS * rel_c, 0, STEPS - 1)))


def down_spec(rel_c):
    return pl.BlockSpec((FT, HF), lambda f: (jnp.clip(f - STEPS * rel_c, 0, STEPS - 1), 0))


FFN_W_SPECS = [up_spec(0), up_spec(1)] * 2 + [down_spec(0), down_spec(1)] * 2


def ffn_fwd_kernel(rc, mid_ref, norm_ref, u00, u01, u10, u11, d00, d01, d10, d11, vec, vecu,
                   act_ref, slope_ref, hid_ref, low_ref, n_ref, inv_ref, acc):
    f = pl.program_id(0)

    @pl.when(f == 0)
    def _():
        acc[...] = jnp.zeros_like(acc)

    def step(rel_c, u_near, u_far, d_near, d_far):
        spot = (rc[1] ^ rel_c) * STEPS + f - STEPS * rel_c
        up = dot(mid_ref[0], u_near[...]) + dot(mid_ref[1], u_far[...]) + vecu[spot]
        act, slope = gelu_parts(up)
        act = act.astype(BF16)
        act_ref[...] = act
        slope_ref[...] = slope.astype(BF16)
        acc[0] += dot(act, d_near[...])
        acc[1] += dot(act, d_far[...])

    @pl.when(f < STEPS)
    def _():
        step(0, u00, u10, d00, d10)

    @pl.when(f >= STEPS)
    def _():
        step(1, u01, u11, d01, d11)

    @pl.when(f == 2 * STEPS - 1)
    def _():
        parts = [norm_ref[rel_r] + (acc[rel_r] + vec[6 + (rc[0] ^ rel_r)]) for rel_r in range(2)]
        near, far, inv = norm_pair(*parts)
        for rel_r, n in enumerate((near, far)):
            r = rc[0] ^ rel_r
            out = n * vec[12 + r] + vec[14 + r]
            hid_ref[rel_r] = out
            low_ref[rel_r] = out.astype(BF16)
            n_ref[rel_r] = n
        inv_ref[...] = inv


def ffn_forward(rc, mid, normed, ups, downs, va, vb):
    full = whole((2, TOK, HF))
    wide = pl.BlockSpec((TOK, FT), lambda f: (0, f))
    return pl.pallas_call(
        ffn_fwd_kernel,
        grid=(2 * STEPS,),
        in_specs=[SMEM_SPEC, full, full] + FFN_W_SPECS + [whole(va.shape), whole(vb.shape)],
        out_specs=[wide, wide, full, full, full, whole((TOK, 1))],
        out_shape=[
            sds((TOK, 2 * FFC), BF16), sds((TOK, 2 * FFC), BF16), sds((2, TOK, HF), F32),
            sds((2, TOK, HF), BF16), sds((2, TOK, HF), F32), sds((TOK, 1), F32),
        ],
        scratch_shapes=[pltpu.VMEM((2, TOK, HF), F32)],
        compiler_params=params(),
        cost_estimate=cost(4 * TOK * D * 4 * D, 24e6),
        name="ffn_fwd",
    )(rc, mid, normed, *ups, *downs, va, vb)


def put_tiles(ref, lead, first, block):
    rows, cols = block.shape
    spot = first
    for i in range(rows // TILE):
        for j in range(cols // TILE):
            ref[lead + (spot,)] = block[
                i * TILE : (i + 1) * TILE, j * TILE : (j + 1) * TILE
            ].astype(BF16)
            spot += 1


def ffn_bwd_kernel(rc, g_ref, n2_ref, inv2_ref, mid_ref, act_ref, slope_ref, n1_ref, inv1_ref,
                   u00, u01, u10, u11, d00, d01, d10, d11, vec,
                   gm_ref, gt_ref, dres_ref, dbr_ref, gv_ref, gu_ref, d_two, d_down, d_mid):
    f = pl.program_id(0)
    rs = [rc[0], rc[0] ^ 1]

    def note(which, rel_r, value):
        gv_ref[2 * which + rs[rel_r]] = jnp.sum(value, 0, keepdims=True)

    @pl.when(f == 0)
    def _():
        grads = [g_ref[0], g_ref[1]]
        normed = [n2_ref[0], n2_ref[1]]
        d_resid = norm_pair_back(grads, normed, inv2_ref[...], [vec[12 + r] for r in rs])
        for rel_r in range(2):
            note(4, rel_r, grads[rel_r] * normed[rel_r])
            note(5, rel_r, grads[rel_r])
            d_two[rel_r] = d_resid[rel_r]
            low = d_resid[rel_r].astype(BF16)
            d_down[rel_r] = low
            note(1, rel_r, low.astype(F32))
        d_mid[...] = jnp.zeros_like(d_mid)

    def step(rel_c, u_near, u_far, d_near, d_far):
        spot = (rc[1] ^ rel_c) * STEPS + f - STEPS * rel_c
        d_act = dot_bt(d_down[0], d_near[...]) + dot_bt(d_down[1], d_far[...])
        d_up = (d_act * slope_ref[...].astype(F32)).astype(BF16)
        gu_ref[spot] = jnp.sum(d_up.astype(F32), 0, keepdims=True)
        act = act_ref[...]
        for rel_r, (ref, u_piece) in enumerate(((gm_ref, u_near), (gt_ref, u_far))):
            put_tiles(ref, (0, 0), 0, dot_at(mid_ref[rel_r], d_up))
            put_tiles(ref, (0, 0), 12, dot_at(act, d_down[rel_r]))
            d_mid[rel_r] += dot_bt(d_up, u_piece[...])

    @pl.when(f < STEPS)
    def _():
        step(0, u00, u10, d00, d10)

    @pl.when(f >= STEPS)
    def _():
        step(1, u01, u11, d01, d11)

    @pl.when(f == 2 * STEPS - 1)
    def _():
        grads = [d_two[rel_r] + d_mid[rel_r] for rel_r in range(2)]
        normed = [n1_ref[0], n1_ref[1]]
        d_resid = norm_pair_back(grads, normed, inv1_ref[...], [vec[8 + r] for r in rs])
        for rel_r in range(2):
            note(2, rel_r, grads[rel_r] * normed[rel_r])
            note(3, rel_r, grads[rel_r])
            dres_ref[rel_r] = d_resid[rel_r]
            low = d_resid[rel_r].astype(BF16)
            dbr_ref[rel_r] = low
            note(0, rel_r, low.astype(F32))


def ffn_backward(rc, g, n2, inv2, mid, act, slope, n1, inv1, ups, downs, va):
    full = whole((2, TOK, HF))
    col = whole((TOK, 1))
    wide = pl.BlockSpec((TOK, FT), lambda f: (0, f))
    tiles = pl.BlockSpec((1, 1, 24, TILE, TILE), lambda f: (f // STEPS, f % STEPS, 0, 0, 0))
    tile_shape = sds((2, STEPS, 24, TILE, TILE), BF16)
    return pl.pallas_call(
        ffn_bwd_kernel,
        grid=(2 * STEPS,),
        in_specs=[SMEM_SPEC, full, full, col, full, wide, wide, full, col]
        + FFN_W_SPECS
        + [whole(va.shape)],
        out_specs=[tiles, tiles, full, full, whole((12, 1, HF)), whole((2 * STEPS, 1, FT))],
        out_shape=[
            tile_shape, tile_shape, sds((2, TOK, HF), F32), sds((2, TOK, HF), BF16),
            sds((12, 1, HF), F32), sds((2 * STEPS, 1, FT), F32),
        ],
        scratch_shapes=[
            pltpu.VMEM((2, TOK, HF), F32), pltpu.VMEM((2, TOK, HF), BF16),
            pltpu.VMEM((2, TOK, HF), F32),
        ],
        compiler_params=params(),
        cost_estimate=cost(8 * TOK * D * 4 * D, 36e6),
        name="ffn_bwd",
    )(rc, g, n2, inv2, mid, act, slope, n1, inv1, *ups, *downs, va)


def out_bwd_kernel(rc, dbr_ref, a_ref, w00, w01, w10, w11, da_ref, gm_ref, gt_ref):
    for rel_c, (w_near, w_far) in enumerate(((w00, w10), (w01, w11))):
        c = rc[1] ^ rel_c
        da_ref[c] = (dot_bt(dbr_ref[0], w_near[...]) + dot_bt(dbr_ref[1], w_far[...])).astype(BF16)
        rows = a_ref[c]
        put_tiles(gm_ref, (rel_c,), 0, dot_at(rows, dbr_ref[0]))
        put_tiles(gt_ref, (rel_c,), 0, dot_at(rows, dbr_ref[1]))


def out_backward(rc, d_branch, attended, pieces):
    full = whole((2, TOK, HF))
    tiles = (2, 9, TILE, TILE)
    return pl.pallas_call(
        out_bwd_kernel,
        grid=(1,),
        in_specs=[SMEM_SPEC, full, full] + [whole((HF, HF))] * 4,
        out_specs=[full, whole(tiles), whole(tiles)],
        out_shape=[sds((2, TOK, HF), BF16), sds(tiles, BF16), sds(tiles, BF16)],
        compiler_params=params(),
        cost_estimate=cost(4 * TOK * D * D, 6e6),
        name="out_bwd",
    )(rc, d_branch, attended, *pieces)


def qkv_bwd_kernel(rc, dq_ref, own_ref, left_ref, right_ref, dres_ref, x_ref, w00, w01, w10, w11,
                   dx_ref, gm_ref, gt_ref, gv_ref):
    d_near = dres_ref[0]
    d_far = dres_ref[1]
    for rel_c, (w_near, w_far) in enumerate(((w00, w10), (w01, w11))):
        c = rc[1] ^ rel_c
        parts = [dq_ref[c]]
        for which in range(2):
            back = left_ref[c, which].astype(F32) + right_ref[c, which].astype(F32)
            parts.append((own_ref[c, which] + back).astype(BF16))
        gv_ref[c] = jnp.sum(parts[0].astype(F32), 0, keepdims=True)
        gv_ref[2 + c] = jnp.sum(parts[2].astype(F32), 0, keepdims=True)
        for which in range(3):
            span = slice(which * HF, (which + 1) * HF)
            d_near += dot_bt(parts[which], w_near[:, span])
            d_far += dot_bt(parts[which], w_far[:, span])
            put_tiles(gm_ref, (rel_c,), 9 * which, dot_at(x_ref[0], parts[which]))
            put_tiles(gt_ref, (rel_c,), 9 * which, dot_at(x_ref[1], parts[which]))
    dx_ref[0] = d_near
    dx_ref[1] = d_far


def qkv_backward(rc, dq, own, left, right, d_resid, x, pieces):
    full = whole((2, TOK, HF))
    wide = whole((2, 2, TOK, HF))
    tiles = (2, 27, TILE, TILE)
    return pl.pallas_call(
        qkv_bwd_kernel,
        grid=(1,),
        in_specs=[SMEM_SPEC, full, wide, wide, wide, full, full] + [whole((HF, 3 * HF))] * 4,
        out_specs=[full, whole(tiles), whole(tiles), whole((4, 1, HF))],
        out_shape=[sds((2, TOK, HF), F32), sds(tiles, BF16), sds(tiles, BF16), sds((4, 1, HF), F32)],
        compiler_params=params(),
        cost_estimate=cost(12 * TOK * D * D, 20e6),
        name="qkv_bwd",
    )(rc, dq, own, left, right, d_resid, x, *pieces)


def row_swap(value):
    return lax.ppermute(value, "row", SWAP)


def col_swap(value):
    return lax.ppermute(value, "col", SWAP)


def four_pieces(local):
    other = col_swap(local)
    return local, other, row_swap(local), row_swap(other)


LINE_UP = ((0, 2), (2, 1), (1, 3))
LINE_DOWN = ((2, 0), (1, 2), (3, 1))


def send_up(value):
    return lax.ppermute(value, ("row", "col"), LINE_UP)


def send_down(value):
    return lax.ppermute(value, ("row", "col"), LINE_DOWN)


def add_low(*values):
    total = values[0].astype(F32)
    for value in values[1:]:
        total = total + value.astype(F32)
    return total.astype(BF16)


def pick(pair, bit):
    return lax.dynamic_index_in_dim(pair, bit, 0, keepdims=False)


def join_by(bit, near, far):
    return jnp.where(
        bit == 0, jnp.concatenate((near, far), 0), jnp.concatenate((far, near), 0)
    )


def reduce_tiles(mine, theirs):
    got = row_swap(theirs)
    away = col_swap(add_low(mine[1], got[1]))
    value = add_low(mine[0], got[0], away)
    count = value.size // (TILE * TILE)
    value = value.reshape(count * TILE, TILE)
    size = lax.axis_size("dp")
    me = lax.axis_index("dp")
    steps = []
    step = 1
    while step < size:
        steps.append(step)
        step *= 2
    for step in steps:
        bit = (me // step) % 2
        pair = value.reshape(2, value.shape[0] // 2, TILE)
        swap = [(i, i ^ step) for i in range(size)]
        value = add_low(pick(pair, bit), lax.ppermute(pick(pair, 1 - bit), "dp", swap))
    for step in reversed(steps):
        bit = (me // step) % 2
        swap = [(i, i ^ step) for i in range(size)]
        value = join_by(bit, value, lax.ppermute(value, "dp", swap))
    return value.reshape(count, TILE, TILE)


def reduce_small(value):
    value = value + row_swap(value)
    value = value + col_swap(value)
    size = lax.axis_size("dp")
    step = 1
    while step < size:
        value = value + lax.ppermute(value, "dp", [(i, i ^ step) for i in range(size)])
        step *= 2
    return value


def tile_places():
    places = []
    for layer in range(LAYERS):
        base = 108 * layer
        places += [base + i for i in range(36)]
        for rt in range(3):
            for ct in range(12):
                places.append(base + 36 + (ct // 4) * 24 + rt * 4 + ct % 4)
        for rt in range(12):
            for ct in range(3):
                places.append(base + 36 + (rt // 4) * 24 + 12 + (rt % 4) * 3 + ct)
    return places


def rotate_update(grad_tiles, left_basis, right_basis, old_m, old_v):
    turned = jnp.einsum("...ji,...jk->...ik", left_basis, grad_tiles, precision=HIGHEST)
    rotated = jnp.einsum("...ik,...kl->...il", turned, right_basis, precision=HIGHEST)
    new_m = DECAY * old_m + (1.0 - DECAY) * rotated
    new_v = DECAY * old_v + (1.0 - DECAY) * rotated * rotated
    direction = new_m / (jnp.sqrt(new_v) + ADAM_EPS)
    back_turn = jnp.einsum("...ij,...jk->...ik", left_basis, direction, precision=HIGHEST)
    update = -TILE_RATE * jnp.einsum(
        "...ik,...lk->...il", back_turn, right_basis, precision=HIGHEST
    )
    return (new_m, new_v, update)


def body(
    tokens, cotangent, segments, valid, w_query, w_key, w_value, w_out, w_up, w_down,
    vectors, vector_m, vector_v, tile_order, basis_left, basis_right, tile_m, tile_v,
):
    r = lax.axis_index("row")
    c = lax.axis_index("col")
    rc = jnp.stack((r, c)).astype(jnp.int32)

    def to_tokens(block):
        pair = block[0].reshape(2, TOK, HF)
        return jnp.stack((pick(pair, r), row_swap(pick(pair, 1 - r))), 0)

    def to_block(pair):
        return join_by(r, pair[0], row_swap(pair[1]))[None]

    x = to_tokens(tokens)
    qkv_w = [
        four_pieces(jnp.concatenate((w_query[layer], w_key[layer], w_value[layer]), 1))
        for layer in range(LAYERS)
    ]
    out_w = [four_pieces(w_out[layer]) for layer in range(LAYERS)]
    up_w = [four_pieces(w_up[layer]) for layer in range(LAYERS)]
    down_w = [four_pieces(w_down[layer]) for layer in range(LAYERS)]

    seg_full = join_by(r, segments[0], row_swap(segments[0]))
    edge = jnp.full((TOK,), -1, jnp.int32)
    seg_ext = lax.dynamic_slice_in_dim(
        jnp.concatenate((edge, seg_full, edge)), (2 * c + r) * TOK, 3 * TOK, 0
    )
    segq = seg_ext[TOK : 2 * TOK].reshape(TOK // QB, 1, QB)
    segk = seg_ext.reshape(3 * TOK, 1)
    keep = lax.dynamic_slice_in_dim(valid[0], r * TOK, TOK, 0).astype(F32).reshape(TOK, 1)
    vas = [vectors[layer, : 8 * D].reshape(16, 1, HF) for layer in range(LAYERS)]
    vbs = [vectors[layer, 8 * D :].reshape(2 * STEPS, 1, FT) for layer in range(LAYERS)]

    hidden = x
    kept = []
    stats = None
    for layer in range(LAYERS):
        q, kv = qkv_forward(rc, x, qkv_w[layer], vas[layer])
        left = send_up(kv)
        right = send_down(kv)
        attended, lse = attn_forward(segk, segq, q, kv, left, right)
        normed, mid, n1, inv1, stat = out_forward(
            rc, attended, out_w[layer], hidden, keep, vas[layer]
        )
        if layer == 0:
            stats = stat
        act, slope, hidden, x_next, n2, inv2 = ffn_forward(
            rc, mid, normed, up_w[layer], down_w[layer], vas[layer], vbs[layer]
        )
        kept.append((x, q, kv, left, right, attended, lse, mid, n1, inv1, act, slope, n2, inv2))
        x = x_next
    final_out = to_block(x)

    grad = to_tokens(cotangent).astype(F32) * keep[None]
    vec_grads = [None] * LAYERS
    tiles = [None] * LAYERS
    for layer in reversed(range(LAYERS)):
        x, q, kv, left, right, attended, lse, mid, n1, inv1, act, slope, n2, inv2 = kept[layer]
        ffn_m, ffn_t, d_resid, d_branch, gv_mid, gv_up = ffn_backward(
            rc, grad, n2, inv2, mid, act, slope, n1, inv1, up_w[layer], down_w[layer], vas[layer]
        )
        d_att, out_m, out_t = out_backward(rc, d_branch, attended, out_w[layer])
        dq, d_left, d_own, d_right = attn_backward(segk, segq, q, d_att, lse, kv, left, right)
        from_left = send_up(d_right)
        from_right = send_down(d_left)
        grad, qkv_m, qkv_t, gv_qkv = qkv_backward(
            rc, dq, d_own, from_left, from_right, d_resid, x, qkv_w[layer]
        )
        tiles[layer] = (
            reduce_tiles(qkv_m, qkv_t),
            reduce_tiles(out_m, out_t),
            reduce_tiles(
                ffn_m.reshape(2, 72, TILE, TILE), ffn_t.reshape(2, 72, TILE, TILE)
            ),
        )
        vec_grads[layer] = jnp.concatenate(
            (gv_qkv.reshape(-1), gv_mid.reshape(-1), gv_up.reshape(-1))
        )
    grad_tokens = to_block(grad)

    vec_len = vectors.shape[1]
    count = jnp.sum(keep) * 1.0
    extra = jnp.stack((jnp.sum(stats[0]), jnp.sum(stats[1]), count))
    late = reduce_small(vec_grads[0])
    early = reduce_small(jnp.concatenate((vec_grads[1], extra, jnp.zeros((125,), F32))))
    vector_grad = jnp.stack((late, early[:vec_len]), 0)
    totals = early[vec_len : vec_len + 3]
    statistics = jnp.sqrt(totals[:2] / (D * totals[2]))

    owner_code = tile_order[0, 0]
    slots = tile_m.shape[2]
    owners = lax.axis_size("dp")
    targets = owner_code % owners * slots + owner_code // owners
    my_slots = lax.axis_index("dp") * slots + jnp.arange(slots)
    match = targets[None, :] == my_slots[:, None]
    places = jnp.asarray(tile_places(), jnp.int32)
    spot = jnp.sum(jnp.where(match, places[None, :], 0), 1)
    taken = jnp.any(match, 1)
    all_tiles = jnp.concatenate(tiles[0] + tiles[1], 0)
    tile_grad = jnp.where(
        taken[:, None, None], jnp.take(all_tiles, spot, axis=0).astype(F32), 0.0
    )

    vector_m_new = DECAY * vector_m + (1.0 - DECAY) * vector_grad
    vector_v_new = DECAY * vector_v + (1.0 - DECAY) * vector_grad * vector_grad
    vector_update = -VECTOR_RATE * vector_m_new / (jnp.sqrt(vector_v_new) + ADAM_EPS)
    tile_m_new, tile_v_new, tile_update = rotate_update(
        tile_grad, basis_left[0, 0], basis_right[0, 0], tile_m[0, 0], tile_v[0, 0]
    )
    return (
        final_out,
        grad_tokens,
        statistics,
        vector_grad,
        vector_m_new,
        vector_v_new,
        vector_update,
        tile_grad[None, None],
        tile_m_new[None, None],
        tile_v_new[None, None],
        tile_update[None, None],
    )


def solution(mesh):
    weight_rc = P(None, "row", "col")
    weight_cr = P(None, "col", "row")
    slot = P("row", "col", "dp", None, None)
    block = P("dp", "col", "row")
    in_specs = (
        block, block, P("dp", "row"), P("dp", "col"),
        weight_rc, weight_rc, weight_rc, weight_cr, weight_rc, weight_cr,
        P(), P(), P(), P("row", "col", None), slot, slot, slot, slot,
    )
    out_specs = (block, block, P(), P(), P(), P(), P(), slot, slot, slot, slot)
    return jax.shard_map(body, mesh=mesh, in_specs=in_specs, out_specs=out_specs, check_vma=False)
```

```python
import functools

import jax
import jax.numpy as jnp
from jax import lax
from jax.experimental import pallas as pl
from jax.experimental.pallas import tpu as pltpu
from jax.sharding import PartitionSpec as P

D = 768
DH = 64
LAYERS = 2
HALF = 512
TILE = 128
HF = 384
FFC = 1536
FT = 512
STEPS = FFC // FT
TOK = 512
QB = 128
KSPAN = QB + 2 * HALF
PAIRS = 3

HIGHEST = lax.Precision.HIGHEST
NEG_BIG = -1e30
NORM_EPS = 1e-06
ADAM_EPS = 1e-08
TILE_RATE = 0.03
VECTOR_RATE = 0.1
DECAY = 0.5
F32 = jnp.float32
BF16 = jnp.bfloat16
SWAP = ((0, 1), (1, 0))


def dot(a, b):
    return lax.dot_general(a, b, (((1,), (0,)), ((), ())), preferred_element_type=F32)


def dot_bt(a, b):
    return lax.dot_general(a, b, (((1,), (1,)), ((), ())), preferred_element_type=F32)


def dot_at(a, b):
    return lax.dot_general(a, b, (((0,), (0,)), ((), ())), preferred_element_type=F32)


def sds(shape, dtype):
    return jax.ShapeDtypeStruct(shape, dtype)


def whole(shape):
    return pl.BlockSpec(shape, lambda *_: (0,) * len(shape))


SMEM_SPEC = pl.BlockSpec(memory_space=pltpu.SMEM)


def cost(flops, nbytes):
    return pl.CostEstimate(flops=int(flops), bytes_accessed=int(nbytes), transcendentals=0)


def params():
    return pltpu.CompilerParams(vmem_limit_bytes=60 * 1024 * 1024)


def panels(ref, rows, first, count):
    return jnp.concatenate(
        [ref[(first + i) * rows : (first + i + 1) * rows, :] for i in range(count)], 1
    )


def qkv_kernel(rc, x_ref, w00, w01, w10, w11, vec, q_ref, kv0_ref, kv1_ref):
    for rel_c, (w_near, w_far) in enumerate(((w00, w10), (w01, w11))):
        c = rc[1] ^ rel_c
        parts = []
        for which in range(3):
            parts.append(
                dot(x_ref[0], panels(w_near, HF, 3 * which, 3))
                + dot(x_ref[1], panels(w_far, HF, 3 * which, 3))
            )
        q = (parts[0] + vec[c]).astype(BF16)
        q_ref[c] = (q.astype(F32) * DH ** (-0.5)).astype(BF16)
        k = parts[1].astype(BF16)
        v = (parts[2] + vec[2 + c]).astype(BF16)
        for index, ref in enumerate((kv0_ref, kv1_ref)):

            @pl.when(c == index)
            def _():
                ref[0] = k
                ref[1] = v


def qkv_forward(rc, x, pieces, va):
    rows = 256
    kv_spec = pl.BlockSpec((2, rows, HF), lambda i: (0, i, 0))
    return pl.pallas_call(
        qkv_kernel,
        grid=(TOK // rows,),
        in_specs=[SMEM_SPEC, pl.BlockSpec((2, rows, HF), lambda i: (0, i, 0))]
        + [pl.BlockSpec((9 * HF, TILE), lambda i: (0, 0))] * 4
        + [whole((16, 1, HF))],
        out_specs=[pl.BlockSpec((2, rows, HF), lambda i: (0, i, 0)), kv_spec, kv_spec],
        out_shape=[sds((2, TOK, HF), BF16)] + [sds((2, TOK, HF), BF16)] * 2,
        compiler_params=params(),
        cost_estimate=cost(2 * TOK * D * 3 * D, 7e6),
        name="qkv",
    )(rc, x, *pieces, va)


def fill_bias(bias, segk_ref, segq_ref, b):
    off = pl.multiple_of(b * QB, QB)
    seg_k = segk_ref[pl.ds(off, KSPAN), :]
    key = lax.broadcasted_iota(jnp.int32, (KSPAN, QB), 0)
    query = lax.broadcasted_iota(jnp.int32, (KSPAN, QB), 1)
    seen = (seg_k == segq_ref[b]) & (jnp.abs(key - query - HALF) < HALF)
    bias[b] = jnp.where(seen, 0.0, NEG_BIG).astype(F32)


def fill_keys(ext, left, own, right):
    ext[0:TOK] = left[0]
    ext[TOK : 2 * TOK] = own[0]
    ext[2 * TOK :] = right[0]


def split_pair(block):
    lane = lax.broadcasted_iota(jnp.int32, block.shape, 1)
    zero = jnp.zeros_like(block)
    return jnp.concatenate(
        (jnp.where(lane < DH, block, zero), jnp.where(lane >= DH, block, zero)), 0
    )


def join_pair(turned):
    return jnp.concatenate((turned[:DH, :QB], turned[DH:, QB:]), 0)


def attn_fwd_kernel(
    segk_ref, segq_ref, q_ref, kl, ko, kr, vl, vo, vr, o_ref, lse_ref, kext, vturn, bias
):
    h = pl.program_id(0)
    b = pl.program_id(1)

    @pl.when(b == 0)
    def _():
        fill_keys(kext, kl, ko, kr)
        for place, part in enumerate((vl, vo, vr)):
            vturn[:, place * TOK : (place + 1) * TOK] = part[0].T

    @pl.when(h == 0)
    def _():
        fill_bias(bias, segk_ref, segq_ref, b)

    off = pl.multiple_of(b * QB, QB)
    qz = split_pair(q_ref[0])
    scores = dot_bt(kext[pl.ds(off, KSPAN), :], qz)
    extra = bias[b]
    scores = scores + jnp.concatenate((extra, extra), 1)
    top = jnp.max(scores, 0, keepdims=True)
    weights = jnp.exp(scores - top)
    total = jnp.sum(weights, 0, keepdims=True)
    turned = dot(vturn[:, pl.ds(off, KSPAN)], weights.astype(BF16)) / total
    o_ref[...] = join_pair(turned).T.astype(BF16)
    lse_ref[0, 0] = top + jnp.log(total)


def pair_specs(c):
    def kv_spec(which):
        return pl.BlockSpec((1, TOK, TILE), lambda h, b: (which, 0, h))

    q_spec = pl.BlockSpec((1, QB, TILE), lambda h, b: (c, b, h))
    o_spec = pl.BlockSpec((QB, TILE), lambda h, b: (b, h))
    lse_spec = pl.BlockSpec((1, 1, 1, 2 * QB), lambda h, b: (h, b, 0, 0))
    return q_spec, o_spec, kv_spec(0), kv_spec(1), lse_spec


def attn_forward(c, segk, segq, q, kv, left, right):
    q_spec, o_spec, k_spec, v_spec, lse_spec = pair_specs(c)
    return pl.pallas_call(
        attn_fwd_kernel,
        grid=(PAIRS, TOK // QB),
        in_specs=[whole(segk.shape), whole(segq.shape), q_spec] + [k_spec] * 3 + [v_spec] * 3,
        out_specs=[o_spec, lse_spec],
        out_shape=[sds((TOK, HF), BF16), sds((PAIRS, TOK // QB, 1, 2 * QB), F32)],
        scratch_shapes=[
            pltpu.VMEM((3 * TOK, TILE), BF16),
            pltpu.VMEM((TILE, 3 * TOK), BF16),
            pltpu.VMEM((TOK // QB, KSPAN, QB), F32),
        ],
        compiler_params=params(),
        cost_estimate=cost(8e9, 4e6),
        name="attn_fwd",
    )(segk, segq, q, left, kv, right, left, kv, right)


def attn_bwd_kernel(
    segk_ref, segq_ref, q_ref, g_ref, lse_ref, kl, ko, kr, vl, vo, vr,
    dq_ref, dl_ref, do_ref, dr_ref, kext, vext, kturn, bias, dk, dv,
):
    h = pl.program_id(0)
    b = pl.program_id(1)

    @pl.when(b == 0)
    def _():
        fill_keys(kext, kl, ko, kr)
        fill_keys(vext, vl, vo, vr)
        for place, part in enumerate((kl, ko, kr)):
            kturn[:, place * TOK : (place + 1) * TOK] = part[0].T
        dk[...] = jnp.zeros_like(dk)
        dv[...] = jnp.zeros_like(dv)

    @pl.when(h == 0)
    def _():
        fill_bias(bias, segk_ref, segq_ref, b)

    off = pl.multiple_of(b * QB, QB)
    span = pl.ds(off, KSPAN)
    qz = split_pair(q_ref[0])
    gz = split_pair(g_ref[0])
    scores = dot_bt(kext[span, :], qz)
    extra = bias[b]
    weights = jnp.exp(scores + jnp.concatenate((extra, extra), 1) - lse_ref[0, 0])
    d_weights = dot_bt(vext[span, :], gz)
    row_dot = jnp.sum(weights * d_weights, 0, keepdims=True)
    d_scores = (weights * (d_weights - row_dot)).astype(BF16)
    dv[span, :] += dot(weights.astype(BF16), gz)
    dk[span, :] += dot(d_scores, qz)
    turned = dot(kturn[:, span], d_scores)
    dq_ref[...] = (join_pair(turned).T * DH ** (-0.5)).astype(BF16)

    @pl.when(b == TOK // QB - 1)
    def _():
        for which, grads in enumerate((dk, dv)):
            dl_ref[which] = grads[0:TOK].astype(BF16)
            do_ref[which] = grads[TOK : 2 * TOK]
            dr_ref[which] = grads[2 * TOK :].astype(BF16)


def attn_backward(c, segk, segq, q, g, lse, kv, left, right):
    q_spec, o_spec, k_spec, v_spec, lse_spec = pair_specs(c)
    d_spec = pl.BlockSpec((2, TOK, TILE), lambda h, b: (0, 0, h))
    d_shape = (2, TOK, HF)
    return pl.pallas_call(
        attn_bwd_kernel,
        grid=(PAIRS, TOK // QB),
        in_specs=[whole(segk.shape), whole(segq.shape), q_spec, q_spec, lse_spec]
        + [k_spec] * 3
        + [v_spec] * 3,
        out_specs=[o_spec, d_spec, d_spec, d_spec],
        out_shape=[
            sds((TOK, HF), BF16), sds(d_shape, BF16), sds(d_shape, F32), sds(d_shape, BF16),
        ],
        scratch_shapes=[
            pltpu.VMEM((3 * TOK, TILE), BF16),
            pltpu.VMEM((3 * TOK, TILE), BF16),
            pltpu.VMEM((TILE, 3 * TOK), BF16),
            pltpu.VMEM((TOK // QB, KSPAN, QB), F32),
            pltpu.VMEM((3 * TOK, TILE), F32),
            pltpu.VMEM((3 * TOK, TILE), F32),
        ],
        compiler_params=params(),
        cost_estimate=cost(15e9, 8e6),
        name="attn_bwd",
    )(segk, segq, q, g, lse, left, kv, right, left, kv, right)


def feature_sum(near, far):
    return jnp.sum(near, 1, keepdims=True) + jnp.sum(far, 1, keepdims=True)


def norm_pair(near, far):
    mean = feature_sum(near, far) / D
    near = near - mean
    far = far - mean
    inv = lax.rsqrt(feature_sum(near * near, far * far) / D + NORM_EPS)
    return near * inv, far * inv, inv


def norm_pair_back(grads, normed, inv, gains):
    dn = [g * gain for g, gain in zip(grads, gains)]
    first = feature_sum(*dn) / D
    second = feature_sum(*[d * n for d, n in zip(dn, normed)]) / D
    return [inv * (d - first - n * second) for d, n in zip(dn, normed)]


def out_kernel(rc, a0_ref, a1_ref, w00, w01, w10, w11, hid_ref, valid_ref, vec,
               norm_ref, mid_ref, n_ref, inv_ref, stat_ref):
    keep = valid_ref[...]
    first = rc[1] == 0
    a_near = jnp.where(first, a0_ref[...], a1_ref[...])
    a_far = jnp.where(first, a1_ref[...], a0_ref[...])
    resid = []
    sums = []
    for rel_r, (w_near, w_far) in enumerate(((w00, w01), (w10, w11))):
        r = rc[0] ^ rel_r
        branch = (
            dot(a_near, panels(w_near, HF, 0, 3)) + dot(a_far, panels(w_far, HF, 0, 3)) + vec[4 + r]
        )
        total = hid_ref[rel_r].astype(F32) + branch
        resid.append(total)
        sums.append((total * total, branch * branch))

    @pl.when(pl.program_id(0) == 0)
    def _():
        stat_ref[...] = jnp.zeros_like(stat_ref)

    for which in range(2):
        part = (sums[0][which] + sums[1][which]) * keep
        stat_ref[which] += jnp.sum(part, 0, keepdims=True)
    near, far, inv = norm_pair(*resid)
    for rel_r, n in enumerate((near, far)):
        r = rc[0] ^ rel_r
        out = n * vec[8 + r] + vec[10 + r]
        norm_ref[rel_r] = out
        mid_ref[rel_r] = out.astype(BF16)
        n_ref[rel_r] = n
    inv_ref[...] = inv


def out_spec(spot):
    return pl.BlockSpec((3 * HF, TILE), lambda *_: (spot, 0))


def out_forward(rc, attended, pieces, spot, hidden, valid, va):
    rows = 256
    head = pl.BlockSpec((rows, HF), lambda i: (i, 0))
    half = pl.BlockSpec((2, rows, HF), lambda i: (0, i, 0))
    col = pl.BlockSpec((rows, 1), lambda i: (i, 0))
    return pl.pallas_call(
        out_kernel,
        grid=(TOK // rows,),
        in_specs=[SMEM_SPEC, head, head] + [out_spec(spot)] * 4 + [half, col, whole((16, 1, HF))],
        out_specs=[half, half, half, col, whole((2, 1, HF))],
        out_shape=[
            sds((2, TOK, HF), F32), sds((2, TOK, HF), BF16), sds((2, TOK, HF), F32),
            sds((TOK, 1), F32), sds((2, 1, HF), F32),
        ],
        compiler_params=params(),
        cost_estimate=cost(2 * TOK * D * D, 7e6),
        name="attn_out",
    )(rc, *attended, *pieces, hidden, valid, va)


def gelu_parts(u):
    bell = jnp.exp(-0.5 * u * u)
    t = 1.0 / (1.0 + (0.3275911 * 0.7071067811865476) * jnp.abs(u))
    poly = t * (0.5 * 0.254829592 + t * (0.5 * -0.284496736 + t * (
        0.5 * 1.421413741 + t * (0.5 * -1.453152027 + t * (0.5 * 1.061405429)))))
    tail = poly * bell
    below = jnp.where(u >= 0, 1.0 - tail, tail)
    return u * below, below + u * bell * 0.3989422804014327


def ffn_specs(base):
    def spec(rel_c):
        return pl.BlockSpec(
            (STEPS * FT, TILE),
            lambda f: (base + jnp.clip(f - STEPS * rel_c, 0, STEPS - 1), 0),
        )

    return [spec(0), spec(1)] * 2


def up_tile(ref):
    return panels(ref, HF, 0, FT // TILE)


def down_tile(ref):
    return panels(ref, FT, 0, HF // TILE)


def ffn_fwd_kernel(rc, mid_ref, norm_ref, u00, u01, u10, u11, d00, d01, d10, d11, vec, vecu,
                   act_ref, slope_ref, hid_ref, low_ref, n_ref, inv_ref, acc):
    f = pl.program_id(0)

    @pl.when(f == 0)
    def _():
        acc[...] = jnp.zeros_like(acc)

    def step(rel_c, u_near, u_far, d_near, d_far):
        spot = (rc[1] ^ rel_c) * STEPS + f - STEPS * rel_c
        up = dot(mid_ref[0], up_tile(u_near)) + dot(mid_ref[1], up_tile(u_far)) + vecu[spot]
        act, slope = gelu_parts(up)
        act = act.astype(BF16)
        act_ref[...] = act
        slope_ref[...] = slope.astype(BF16)
        acc[0] += dot(act, down_tile(d_near))
        acc[1] += dot(act, down_tile(d_far))

    @pl.when(f < STEPS)
    def _():
        step(0, u00, u10, d00, d10)

    @pl.when(f >= STEPS)
    def _():
        step(1, u01, u11, d01, d11)

    @pl.when(f == 2 * STEPS - 1)
    def _():
        parts = [norm_ref[rel_r] + (acc[rel_r] + vec[6 + (rc[0] ^ rel_r)]) for rel_r in range(2)]
        near, far, inv = norm_pair(*parts)
        for rel_r, n in enumerate((near, far)):
            r = rc[0] ^ rel_r
            out = n * vec[12 + r] + vec[14 + r]
            hid_ref[rel_r] = out
            low_ref[rel_r] = out.astype(BF16)
            n_ref[rel_r] = n
        inv_ref[...] = inv


def ffn_forward(rc, mid, normed, ups, up_base, downs, down_base, va, vb):
    full = whole((2, TOK, HF))
    wide = pl.BlockSpec((TOK, FT), lambda f: (0, f))
    return pl.pallas_call(
        ffn_fwd_kernel,
        grid=(2 * STEPS,),
        in_specs=[SMEM_SPEC, full, full]
        + ffn_specs(up_base)
        + ffn_specs(down_base)
        + [whole(va.shape), whole(vb.shape)],
        out_specs=[wide, wide, full, full, full, whole((TOK, 1))],
        out_shape=[
            sds((TOK, 2 * FFC), BF16), sds((TOK, 2 * FFC), BF16), sds((2, TOK, HF), F32),
            sds((2, TOK, HF), BF16), sds((2, TOK, HF), F32), sds((TOK, 1), F32),
        ],
        scratch_shapes=[pltpu.VMEM((2, TOK, HF), F32)],
        compiler_params=params(),
        cost_estimate=cost(4 * TOK * D * 4 * D, 24e6),
        name="ffn_fwd",
    )(rc, mid, normed, *ups, *downs, va, vb)


def put_tiles(ref, lead, first, block):
    rows, cols = block.shape
    spot = first
    for i in range(rows // TILE):
        for j in range(cols // TILE):
            ref[lead + (spot,)] = block[
                i * TILE : (i + 1) * TILE, j * TILE : (j + 1) * TILE
            ].astype(BF16)
            spot += 1


def ffn_bwd_kernel(rc, g_ref, n2_ref, inv2_ref, mid_ref, act_ref, slope_ref, n1_ref, inv1_ref,
                   u00, u01, u10, u11, d00, d01, d10, d11, vec,
                   gm_ref, gt_ref, dres_ref, dbr_ref, gv_ref, gu_ref, d_two, d_down, d_mid):
    f = pl.program_id(0)
    rs = [rc[0], rc[0] ^ 1]

    def note(which, rel_r, value):
        gv_ref[2 * which + rs[rel_r]] = jnp.sum(value, 0, keepdims=True)

    @pl.when(f == 0)
    def _():
        grads = [g_ref[0], g_ref[1]]
        normed = [n2_ref[0], n2_ref[1]]
        d_resid = norm_pair_back(grads, normed, inv2_ref[...], [vec[12 + r] for r in rs])
        for rel_r in range(2):
            note(4, rel_r, grads[rel_r] * normed[rel_r])
            note(5, rel_r, grads[rel_r])
            d_two[rel_r] = d_resid[rel_r]
            low = d_resid[rel_r].astype(BF16)
            d_down[rel_r] = low
            note(1, rel_r, low.astype(F32))
        d_mid[...] = jnp.zeros_like(d_mid)

    def step(rel_c, u_near, u_far, d_near, d_far):
        spot = (rc[1] ^ rel_c) * STEPS + f - STEPS * rel_c
        d_act = dot_bt(d_down[0], down_tile(d_near)) + dot_bt(d_down[1], down_tile(d_far))
        d_up = (d_act * slope_ref[...].astype(F32)).astype(BF16)
        gu_ref[spot] = jnp.sum(d_up.astype(F32), 0, keepdims=True)
        act = act_ref[...]
        for rel_r, (ref, u_piece) in enumerate(((gm_ref, u_near), (gt_ref, u_far))):
            put_tiles(ref, (0,), 0, dot_at(mid_ref[rel_r], d_up))
            put_tiles(ref, (0,), 12, dot_at(act, d_down[rel_r]))
            d_mid[rel_r] += dot_bt(d_up, up_tile(u_piece))

    @pl.when(f < STEPS)
    def _():
        step(0, u00, u10, d00, d10)

    @pl.when(f >= STEPS)
    def _():
        step(1, u01, u11, d01, d11)

    @pl.when(f == 2 * STEPS - 1)
    def _():
        grads = [d_two[rel_r] + d_mid[rel_r] for rel_r in range(2)]
        normed = [n1_ref[0], n1_ref[1]]
        d_resid = norm_pair_back(grads, normed, inv1_ref[...], [vec[8 + r] for r in rs])
        for rel_r in range(2):
            note(2, rel_r, grads[rel_r] * normed[rel_r])
            note(3, rel_r, grads[rel_r])
            dres_ref[rel_r] = d_resid[rel_r]
            low = d_resid[rel_r].astype(BF16)
            dbr_ref[rel_r] = low
            note(0, rel_r, low.astype(F32))


def ffn_backward(
    rc, g, n2, inv2, mid, act, slope, n1, inv1, ups, up_base, downs, down_base, va
):
    full = whole((2, TOK, HF))
    col = whole((TOK, 1))
    wide = pl.BlockSpec((TOK, FT), lambda f: (0, f))
    tiles = pl.BlockSpec((1, 24, TILE, TILE), lambda f: (f // STEPS, f % STEPS, 0, 0))
    tile_shape = sds((2, 81, TILE, TILE), BF16)
    return pl.pallas_call(
        ffn_bwd_kernel,
        grid=(2 * STEPS,),
        in_specs=[SMEM_SPEC, full, full, col, full, wide, wide, full, col]
        + ffn_specs(up_base)
        + ffn_specs(down_base)
        + [whole(va.shape)],
        out_specs=[tiles, tiles, full, full, whole((12, 1, HF)), whole((2 * STEPS, 1, FT))],
        out_shape=[
            tile_shape, tile_shape, sds((2, TOK, HF), F32), sds((2, TOK, HF), BF16),
            sds((12, 1, HF), F32), sds((2 * STEPS, 1, FT), F32),
        ],
        scratch_shapes=[
            pltpu.VMEM((2, TOK, HF), F32), pltpu.VMEM((2, TOK, HF), BF16),
            pltpu.VMEM((2, TOK, HF), F32),
        ],
        compiler_params=params(),
        cost_estimate=cost(8 * TOK * D * 4 * D, 36e6),
        name="ffn_bwd",
    )(rc, g, n2, inv2, mid, act, slope, n1, inv1, *ups, *downs, va)


def out_bwd_kernel(rc, dbr_ref, a0_ref, a1_ref, w00, w01, w10, w11, gm_in, gt_in,
                   da_ref, gm_ref, gt_ref):
    del gm_in, gt_in
    for rel_c, (w_near, w_far) in enumerate(((w00, w10), (w01, w11))):
        c = rc[1] ^ rel_c
        da_ref[c] = (
            dot_bt(dbr_ref[0], panels(w_near, HF, 0, 3))
            + dot_bt(dbr_ref[1], panels(w_far, HF, 0, 3))
        ).astype(BF16)
        rows = jnp.where(c == 0, a0_ref[...], a1_ref[...])
        put_tiles(gm_ref, (rel_c,), 0, dot_at(rows, dbr_ref[0]))
        put_tiles(gt_ref, (rel_c,), 0, dot_at(rows, dbr_ref[1]))


def out_backward(rc, d_branch, attended, pieces, spot, tiles_m, tiles_t):
    full = whole((2, TOK, HF))
    anywhere = pl.BlockSpec(memory_space=pl.ANY)
    tiles = pl.BlockSpec((2, 9, TILE, TILE), lambda i: (0, 8, 0, 0))
    return pl.pallas_call(
        out_bwd_kernel,
        grid=(1,),
        in_specs=[SMEM_SPEC, full, whole((TOK, HF)), whole((TOK, HF))]
        + [out_spec(spot)] * 4
        + [anywhere, anywhere],
        out_specs=[full, tiles, tiles],
        out_shape=[
            sds((2, TOK, HF), BF16), sds(tiles_m.shape, BF16), sds(tiles_t.shape, BF16),
        ],
        input_output_aliases={8: 1, 9: 2},
        compiler_params=params(),
        cost_estimate=cost(4 * TOK * D * D, 6e6),
        name="out_bwd",
    )(rc, d_branch, *attended, *pieces, tiles_m, tiles_t)


def qkv_bwd_kernel(col, rc, dq_ref, own_ref, left_ref, right_ref, dx_in, x_ref,
                   w00, w01, w10, w11, gm_in, gt_in, dx_ref, gm_ref, gt_ref, gv_ref):
    del gm_in, gt_in
    parts = [dq_ref[...]]
    for which in range(2):
        back = left_ref[which].astype(F32) + right_ref[which].astype(F32)
        parts.append((own_ref[which] + back).astype(BF16))
    gv_ref[0] = jnp.sum(parts[0].astype(F32), 0, keepdims=True)
    gv_ref[1] = jnp.sum(parts[2].astype(F32), 0, keepdims=True)
    for which in range(3):
        put_tiles(gm_ref, (0,), 9 * which, dot_at(x_ref[0], parts[which]))
        put_tiles(gt_ref, (0,), 9 * which, dot_at(x_ref[1], parts[which]))

    def inputs_grad(w_near, w_far):
        for rel_r, w in enumerate((w_near, w_far)):
            total = dx_in[rel_r]
            for which in range(3):
                total += dot_bt(parts[which], panels(w, HF, 3 * which, 3))
            dx_ref[rel_r] = total

    @pl.when(rc[1] == col)
    def _():
        inputs_grad(w00, w10)

    @pl.when(rc[1] != col)
    def _():
        inputs_grad(w01, w11)


def qkv_backward(col, rc, dq, own, left, right, dx, x, pieces, earlier):
    full = pl.BlockSpec((2, TOK, HF), lambda i, s: (0, 0, 0))
    anywhere = pl.BlockSpec(memory_space=pl.ANY)
    tiles = pl.BlockSpec((1, 27, TILE, TILE), lambda i, s: (s[1] ^ col, 0, 0, 0))
    tile_shape = sds((2, 27, TILE, TILE), BF16)
    if earlier is None:
        kernel = lambda rc, *refs: qkv_bwd_kernel(col, rc, *refs[:10], None, None, *refs[10:])
        aliases = {}
        extra = ()
    else:
        kernel = functools.partial(qkv_bwd_kernel, col)
        aliases = {11: 1, 12: 2}
        extra = earlier
    return pl.pallas_call(
        kernel,
        grid_spec=pltpu.PrefetchScalarGridSpec(
            num_scalar_prefetch=1,
            grid=(1,),
            in_specs=[pl.BlockSpec((TOK, HF), lambda i, s: (0, 0)), full, full, full, full, full]
            + [pl.BlockSpec((9 * HF, TILE), lambda i, s: (0, 0))] * 4
            + [anywhere] * len(extra),
            out_specs=[full, tiles, tiles, pl.BlockSpec((2, 1, HF), lambda i, s: (0, 0, 0))],
        ),
        out_shape=[sds((2, TOK, HF), F32), tile_shape, tile_shape, sds((2, 1, HF), F32)],
        input_output_aliases=aliases,
        compiler_params=params(),
        cost_estimate=cost(6 * TOK * D * D, 10e6),
        name="qkv_bwd",
    )(rc, dq, own, left, right, dx, x, *pieces, *extra)


def row_swap(value):
    return lax.ppermute(value, "row", SWAP)


def col_swap(value):
    return lax.ppermute(value, "col", SWAP)


def dp_swap(value, step):
    size = lax.axis_size("dp")
    return lax.ppermute(value, "dp", [(i, i ^ step) for i in range(size)])


def put_panels(ref, spot, block, rows):
    height, width = block.shape
    for i in range(height // rows):
        for j in range(width // TILE):
            ref[spot : spot + rows, :] = block[i * rows : (i + 1) * rows, j * TILE : (j + 1) * TILE]
            spot += rows
    return spot


def pack_kernel(plan, halves, rc, *refs):
    inputs = refs[: len(refs) - len(plan) - len(halves)]
    outs = refs[len(inputs) : len(inputs) + len(plan)]
    for out, entries in zip(outs, plan):
        spot = 0
        for which, rows in entries:
            spot = put_panels(out, spot, inputs[which][0], rows)
    for which, half in zip(halves, refs[len(inputs) + len(plan) :]):
        count = half.shape[0]
        half[...] = outs[which][pl.ds(pl.multiple_of(rc[2] * count, 16), count), :]


def pack(rc, weights, plan, halves):
    specs = []
    for array, layer in weights:
        specs.append(pl.BlockSpec((1,) + array.shape[1:], lambda i, layer=layer: (layer, 0, 0)))
    heights = []
    for entries in plan:
        heights.append(sum(weights[w][0].shape[1] * weights[w][0].shape[2] for w, _ in entries) // TILE)
    shapes = [sds((h, TILE), BF16) for h in heights]
    shapes += [sds((heights[w] // 2, TILE), BF16) for w in halves]
    return pl.pallas_call(
        functools.partial(pack_kernel, plan, halves),
        grid=(1,),
        in_specs=[SMEM_SPEC] + specs,
        out_specs=[whole(shape.shape) for shape in shapes],
        out_shape=shapes,
        compiler_params=params(),
        cost_estimate=cost(1e6, 3 * TILE * 2 * sum(heights)),
        name="pack",
    )(rc, *[array for array, _ in weights])


def tie(value, *others):
    return lax.optimization_barrier((value, others))


def four_pieces(local, half, after):
    if half is None:
        near = col_swap(local if after is None else tie(local, after)[0])
        other = near
    else:
        near = col_swap(half if after is None else tie(half, after)[0])
        other = join_by(lax.axis_index("dp") % 2, near, dp_swap(near, 1))
    return (local, other, row_swap(local), row_swap(other)), near


LINE_UP = ((0, 2), (2, 1), (1, 3))
LINE_DOWN = ((2, 0), (1, 2), (3, 1))


def send_up(value):
    return lax.ppermute(value, ("row", "col"), LINE_UP)


def send_down(value):
    return lax.ppermute(value, ("row", "col"), LINE_DOWN)


def add_low(*values):
    total = values[0].astype(F32)
    for value in values[1:]:
        total = total + value.astype(F32)
    return total.astype(BF16)


def pick(pair, bit):
    return lax.dynamic_index_in_dim(pair, bit, 0, keepdims=False)


def join_by(bit, near, far):
    return jnp.where(
        bit == 0, jnp.concatenate((near, far), 0), jnp.concatenate((far, near), 0)
    )


def split_rows(value, step):
    bit = (lax.axis_index("dp") // step) % 2
    pair = value.reshape(value.shape[0], 2, value.shape[1] // 2, TILE)
    keep = lax.dynamic_index_in_dim(pair, bit, 1, keepdims=False)
    away = lax.dynamic_index_in_dim(pair, 1 - bit, 1, keepdims=False)
    return keep, away


def reduce_steps(mine, theirs, col_first):
    count = mine.shape[1]
    got = yield row_swap(theirs)
    if col_first:
        away = add_low(mine[1], got[1])
        keep = add_low(mine[0], got[0])
        value = add_low(keep, (yield col_swap(away)))
    else:
        value = add_low(mine, got).reshape(2 * count, TILE, TILE)
    step = 1
    while step < lax.axis_size("dp"):
        keep, away = split_rows(value, step)
        value = add_low(keep, (yield dp_swap(away, step)))
        if step == 1 and not col_first:
            value = add_low(value[:count], (yield col_swap(value[count:])))
        step *= 2
    yield value


class Reduction:
    def __init__(self, mine, theirs, col_first):
        self.steps = reduce_steps(mine, theirs, col_first)
        self.left = 2 + lax.axis_size("dp").bit_length() - 1
        self.value = next(self.steps)

    def finish(self):
        while self.left:
            self.value = self.steps.send(self.value)
            self.left -= 1
        return self.value


def advance(value, *reductions):
    live = [red for red in reductions if red.left]
    value, got = tie(value, *[red.value for red in live])
    for red, part in zip(live, got):
        red.value = red.steps.send(part)
        red.left -= 1
    return value


def reduce_small(value):
    value = value + row_swap(value)
    value = value + col_swap(value)
    size = lax.axis_size("dp")
    step = 1
    while step < size:
        value = value + lax.ppermute(value, "dp", [(i, i ^ step) for i in range(size)])
        step *= 2
    return value


def tile_places():
    places = []
    for layer in range(LAYERS):
        base = 108 * layer
        places += [base + 81 + i for i in range(27)]
        places += [base + 72 + i for i in range(9)]
        for rt in range(3):
            for ct in range(12):
                places.append(base + (ct // 4) * 24 + rt * 4 + ct % 4)
        for rt in range(12):
            for ct in range(3):
                places.append(base + (rt // 4) * 24 + 12 + (rt % 4) * 3 + ct)
    return places


def rotate_update(grad_tiles, left_basis, right_basis, old_m, old_v):
    turned = jnp.einsum("...ji,...jk->...ik", left_basis, grad_tiles, precision=HIGHEST)
    rotated = jnp.einsum("...ik,...kl->...il", turned, right_basis, precision=HIGHEST)
    new_m = DECAY * old_m + (1.0 - DECAY) * rotated
    new_v = DECAY * old_v + (1.0 - DECAY) * rotated * rotated
    direction = new_m / (jnp.sqrt(new_v) + ADAM_EPS)
    back_turn = jnp.einsum("...ij,...jk->...ik", left_basis, direction, precision=HIGHEST)
    update = -TILE_RATE * jnp.einsum(
        "...ik,...lk->...il", back_turn, right_basis, precision=HIGHEST
    )
    return (new_m, new_v, update)


def body(
    tokens, cotangent, segments, valid, w_query, w_key, w_value, w_out, w_up, w_down,
    vectors, vector_m, vector_v, tile_order, basis_left, basis_right, tile_m, tile_v,
):
    r = lax.axis_index("row")
    c = lax.axis_index("col")
    rc = jnp.stack((r, c, lax.axis_index("dp") % 2)).astype(jnp.int32)

    def to_tokens(block):
        pair = block[0].reshape(2, TOK, HF)
        return jnp.stack((pick(pair, r), row_swap(pick(pair, 1 - r))), 0)

    def to_block(pair):
        return join_by(r, pair[0], row_swap(pair[1]))[None]

    x = to_tokens(tokens)
    (near_pack,) = pack(
        rc, ((w_query, 0), (w_key, 0), (w_value, 0)), (((0, HF), (1, HF), (2, HF)),), ()
    )
    near_w, near_done = four_pieces(near_pack, None, None)
    packs = pack(
        rc,
        ((w_up, 0), (w_out, 0), (w_down, 0), (w_query, 1), (w_key, 1), (w_value, 1), (w_out, 1),
         (w_up, 1), (w_down, 1)),
        (
            ((0, HF), (1, HF)),
            ((2, FT),),
            ((3, HF), (4, HF), (5, HF), (6, HF)),
            ((7, HF), (8, FT)),
        ),
        (0, 1, 2, 3),
    )
    up_w, up_done = four_pieces(packs[0], packs[4], near_done)
    down_w, down_done = four_pieces(packs[1], packs[5], up_done)
    late_w, late_done = four_pieces(packs[2], packs[6], down_done)
    ffn_w, _ = four_pieces(packs[3], packs[7], late_done)
    qkv_w = (near_w, late_w)
    out_w = ((up_w, 4), (late_w, 3))
    ffn_w = ((up_w, 0, down_w, 0), (ffn_w, 0, ffn_w, 3))

    seg_full = join_by(r, segments[0], row_swap(segments[0]))
    edge = jnp.full((TOK,), -1, jnp.int32)
    seg_ext = lax.dynamic_slice_in_dim(
        jnp.concatenate((edge, seg_full, edge)), (2 * c + r) * TOK, 3 * TOK, 0
    )
    segq = seg_ext[TOK : 2 * TOK].reshape(TOK // QB, 1, QB)
    segk = seg_ext.reshape(3 * TOK, 1)
    keep = lax.dynamic_slice_in_dim(valid[0], r * TOK, TOK, 0).astype(F32).reshape(TOK, 1)
    vas = [vectors[layer, : 8 * D].reshape(16, 1, HF) for layer in range(LAYERS)]
    vbs = [vectors[layer, 8 * D :].reshape(2 * STEPS, 1, FT) for layer in range(LAYERS)]

    hidden = x
    kept = []
    stats = None
    for layer in range(LAYERS):
        q, kv0, kv1 = qkv_forward(rc, x, qkv_w[layer], vas[layer])
        halos = [(send_up(kv0), send_down(kv0))]
        kv1_now, _ = tie(kv1, *halos[0])
        halos.append((send_up(kv1_now), send_down(kv1_now)))
        attended = []
        lse = []
        for col, kv in enumerate((kv0, kv1)):
            out, part = attn_forward(col, segk, segq, q, kv, *halos[col])
            attended.append(out)
            lse.append(part)
        normed, mid, n1, inv1, stat = out_forward(
            rc, attended, *out_w[layer], hidden, keep, vas[layer]
        )
        if layer == 0:
            stats = stat
        act, slope, hidden, x_next, n2, inv2 = ffn_forward(
            rc, mid, normed, *ffn_w[layer], vas[layer], vbs[layer]
        )
        kept.append((x, q, (kv0, kv1), halos, attended, lse, mid, n1, inv1, act, slope, n2, inv2))
        x = x_next
    final_out = to_block(x)

    grad = to_tokens(cotangent).astype(F32) * keep[None]
    vec_grads = [None] * LAYERS
    tiles = [None] * LAYERS
    ffn_red = [None] * LAYERS
    qkv_red = [None] * LAYERS
    for layer in reversed(range(LAYERS)):
        x, q, kvs, halos, attended, lse, mid, n1, inv1, act, slope, n2, inv2 = kept[layer]
        last = layer == 0
        ffn_m, ffn_t, grad, d_branch, gv_mid, gv_up = ffn_backward(
            rc, grad, n2, inv2, mid, act, slope, n1, inv1, *ffn_w[layer], vas[layer]
        )
        if last:
            d_branch = advance(d_branch, ffn_red[1], qkv_red[1])
        d_att, ffn_m, ffn_t = out_backward(
            rc, d_branch, attended, *out_w[layer], ffn_m, ffn_t
        )
        red = Reduction(ffn_m, ffn_t, False)
        ffn_red[layer] = red
        parts = []
        for col in range(2):
            dq, d_left, d_own, d_right = attn_backward(
                col, segk, segq, q, d_att, lse[col], kvs[col], *halos[col]
            )
            parts.append((dq, d_own, send_up(d_right), send_down(d_left)))
            if col == 0:
                d_att, _ = tie(d_att, dq)
                d_att = advance(d_att, red, *((ffn_red[1], qkv_red[1]) if last else ()))
        earlier = None
        gv_qkv = []
        for col in range(2):
            if last:
                grad = advance(grad, ffn_red[1], qkv_red[1])
            grad, qkv_m, qkv_t, gv = qkv_backward(
                col, rc, *parts[col], grad, x, qkv_w[layer], earlier
            )
            earlier = (qkv_m, qkv_t)
            gv_qkv.append(gv)
        qkv_red[layer] = Reduction(qkv_m, qkv_t, True)
        vec_grads[layer] = jnp.concatenate(
            (jnp.stack(gv_qkv, 1).reshape(-1), gv_mid.reshape(-1), gv_up.reshape(-1))
        )
    for layer in range(LAYERS):
        tiles[layer] = (ffn_red[layer].finish(), qkv_red[layer].finish())
    grad_tokens = to_block(grad)

    vec_len = vectors.shape[1]
    extra = jnp.stack((jnp.sum(stats[0]), jnp.sum(stats[1]), jnp.sum(keep)))
    sums = reduce_small(jnp.concatenate((*vec_grads, extra, jnp.zeros((125,), F32))))
    vector_grad = sums[: LAYERS * vec_len].reshape(LAYERS, vec_len)
    totals = sums[LAYERS * vec_len : LAYERS * vec_len + 3]
    statistics = jnp.sqrt(totals[:2] / (D * totals[2]))

    owner_code = tile_order[0, 0]
    slots = tile_m.shape[2]
    owners = lax.axis_size("dp")
    targets = owner_code % owners * slots + owner_code // owners
    match = targets[None, :] == jnp.arange(owners * slots)[:, None]
    places = jnp.asarray(tile_places(), jnp.int32)
    spot = jnp.sum(jnp.where(match, places[None, :], 0), 1)
    taken = lax.dynamic_slice_in_dim(
        jnp.any(match, 1), lax.axis_index("dp") * slots, slots, 0
    )
    all_tiles = jnp.concatenate(tiles[0] + tiles[1], 0)
    rows = TILE // owners
    outbox = jnp.take(all_tiles, spot, axis=0).reshape(owners, slots, rows, TILE)
    inbox = lax.all_to_all(outbox, "dp", 0, 0, tiled=True)
    bits = owners.bit_length() - 1
    inbox = inbox.reshape((2,) * bits + (slots, rows, TILE))
    order = (bits,) + tuple(range(bits - 1, -1, -1)) + (bits + 1, bits + 2)
    tile_grad = inbox.transpose(order).reshape(slots, TILE, TILE).astype(F32)
    tile_grad = jnp.where(taken[:, None, None], tile_grad, 0.0)

    vector_m_new = DECAY * vector_m + (1.0 - DECAY) * vector_grad
    vector_v_new = DECAY * vector_v + (1.0 - DECAY) * vector_grad * vector_grad
    vector_update = -VECTOR_RATE * vector_m_new / (jnp.sqrt(vector_v_new) + ADAM_EPS)
    tile_m_new, tile_v_new, tile_update = rotate_update(
        tile_grad, basis_left[0, 0], basis_right[0, 0], tile_m[0, 0], tile_v[0, 0]
    )
    return (
        final_out,
        grad_tokens,
        statistics,
        vector_grad,
        vector_m_new,
        vector_v_new,
        vector_update,
        tile_grad[None, None],
        tile_m_new[None, None],
        tile_v_new[None, None],
        tile_update[None, None],
    )


def solution(mesh):
    weight_rc = P(None, "row", "col")
    weight_cr = P(None, "col", "row")
    slot = P("row", "col", "dp", None, None)
    block = P("dp", "col", "row")
    in_specs = (
        block, block, P("dp", "row"), P("dp", "col"),
        weight_rc, weight_rc, weight_rc, weight_cr, weight_rc, weight_cr,
        P(), P(), P(), P("row", "col", None), slot, slot, slot, slot,
    )
    out_specs = (block, block, P(), P(), P(), P(), P(), slot, slot, slot, slot)
    return jax.shard_map(body, mesh=mesh, in_specs=in_specs, out_specs=out_specs, check_vma=False)
```

```python
import functools

import jax
import jax.numpy as jnp
from jax import lax
from jax.experimental import pallas as pl
from jax.experimental.pallas import tpu as pltpu
from jax.sharding import PartitionSpec as P

D = 768
DH = 64
LAYERS = 2
HALF = 512
TILE = 128
HF = 384
FFC = 1536
FT = 512
STEPS = FFC // FT
TOK = 512
QB = 128
KSPAN = QB + 2 * HALF
PAIRS = 3

HIGHEST = lax.Precision.HIGHEST
NEG_BIG = -1e30
NORM_EPS = 1e-06
ADAM_EPS = 1e-08
TILE_RATE = 0.03
VECTOR_RATE = 0.1
DECAY = 0.5
F32 = jnp.float32
BF16 = jnp.bfloat16
SWAP = ((0, 1), (1, 0))


def dot(a, b):
    return lax.dot_general(a, b, (((1,), (0,)), ((), ())), preferred_element_type=F32)


def dot_bt(a, b):
    return lax.dot_general(a, b, (((1,), (1,)), ((), ())), preferred_element_type=F32)


def dot_at(a, b):
    return lax.dot_general(a, b, (((0,), (0,)), ((), ())), preferred_element_type=F32)


def sds(shape, dtype):
    return jax.ShapeDtypeStruct(shape, dtype)


def whole(shape):
    return pl.BlockSpec(shape, lambda *_: (0,) * len(shape))


SMEM_SPEC = pl.BlockSpec(memory_space=pltpu.SMEM)


def cost(flops, nbytes):
    return pl.CostEstimate(flops=int(flops), bytes_accessed=int(nbytes), transcendentals=0)


def params():
    return pltpu.CompilerParams(vmem_limit_bytes=60 * 1024 * 1024)


def panels(ref, rows, first, count):
    return jnp.concatenate(
        [ref[(first + i) * rows : (first + i + 1) * rows, :] for i in range(count)], 1
    )


def qkv_kernel(rc, x_ref, w00, w01, w10, w11, vec, q_ref, kv0_ref, kv1_ref):
    for rel_c, (w_near, w_far) in enumerate(((w00, w10), (w01, w11))):
        c = rc[1] ^ rel_c
        parts = []
        for which in range(3):
            parts.append(
                dot(x_ref[0], panels(w_near, HF, 3 * which, 3))
                + dot(x_ref[1], panels(w_far, HF, 3 * which, 3))
            )
        q = (parts[0] + vec[c]).astype(BF16)
        q_ref[c] = (q.astype(F32) * DH ** (-0.5)).astype(BF16)
        k = parts[1].astype(BF16)
        v = (parts[2] + vec[2 + c]).astype(BF16)
        for index, ref in enumerate((kv0_ref, kv1_ref)):

            @pl.when(c == index)
            def _():
                ref[0] = k
                ref[1] = v


def qkv_forward(rc, x, pieces, va):
    rows = 256
    kv_spec = pl.BlockSpec((2, rows, HF), lambda i: (0, i, 0))
    return pl.pallas_call(
        qkv_kernel,
        grid=(TOK // rows,),
        in_specs=[SMEM_SPEC, pl.BlockSpec((2, rows, HF), lambda i: (0, i, 0))]
        + [pl.BlockSpec((9 * HF, TILE), lambda i: (0, 0))] * 4
        + [whole((16, 1, HF))],
        out_specs=[pl.BlockSpec((2, rows, HF), lambda i: (0, i, 0)), kv_spec, kv_spec],
        out_shape=[sds((2, TOK, HF), BF16)] + [sds((2, TOK, HF), BF16)] * 2,
        compiler_params=params(),
        cost_estimate=cost(2 * TOK * D * 3 * D, 7e6),
        name="qkv",
    )(rc, x, *pieces, va)


def fill_bias(bias, segk_ref, segq_ref, b):
    off = pl.multiple_of(b * QB, QB)
    seg_k = segk_ref[pl.ds(off, KSPAN), :]
    key = lax.broadcasted_iota(jnp.int32, (KSPAN, QB), 0)
    query = lax.broadcasted_iota(jnp.int32, (KSPAN, QB), 1)
    seen = (seg_k == segq_ref[b]) & (jnp.abs(key - query - HALF) < HALF)
    bias[b] = jnp.where(seen, 0.0, NEG_BIG).astype(F32)


def fill_keys(ext, left, own, right):
    ext[0:TOK] = left[0]
    ext[TOK : 2 * TOK] = own[0]
    ext[2 * TOK :] = right[0]


def split_pair(block):
    lane = lax.broadcasted_iota(jnp.int32, block.shape, 1)
    zero = jnp.zeros_like(block)
    return jnp.concatenate(
        (jnp.where(lane < DH, block, zero), jnp.where(lane >= DH, block, zero)), 0
    )


def join_pair(turned):
    return jnp.concatenate((turned[:DH, :QB], turned[DH:, QB:]), 0)


def attn_fwd_kernel(
    segk_ref, segq_ref, q_ref, kl, ko, kr, vl, vo, vr, o_ref, lse_ref, kext, vturn, bias
):
    h = pl.program_id(0)
    b = pl.program_id(1)

    @pl.when(b == 0)
    def _():
        fill_keys(kext, kl, ko, kr)
        for place, part in enumerate((vl, vo, vr)):
            vturn[:, place * TOK : (place + 1) * TOK] = part[0].T

    @pl.when(h == 0)
    def _():
        fill_bias(bias, segk_ref, segq_ref, b)

    off = pl.multiple_of(b * QB, QB)
    qz = split_pair(q_ref[0])
    scores = dot_bt(kext[pl.ds(off, KSPAN), :], qz)
    extra = bias[b]
    scores = scores + jnp.concatenate((extra, extra), 1)
    top = jnp.max(scores, 0, keepdims=True)
    weights = jnp.exp(scores - top)
    total = jnp.sum(weights, 0, keepdims=True)
    turned = dot(vturn[:, pl.ds(off, KSPAN)], weights.astype(BF16)) / total
    o_ref[...] = join_pair(turned).T.astype(BF16)
    lse_ref[0, 0] = top + jnp.log(total)


def pair_specs(c):
    def kv_spec(which):
        return pl.BlockSpec((1, TOK, TILE), lambda h, b: (which, 0, h))

    q_spec = pl.BlockSpec((1, QB, TILE), lambda h, b: (c, b, h))
    o_spec = pl.BlockSpec((QB, TILE), lambda h, b: (b, h))
    lse_spec = pl.BlockSpec((1, 1, 1, 2 * QB), lambda h, b: (h, b, 0, 0))
    return q_spec, o_spec, kv_spec(0), kv_spec(1), lse_spec


def attn_forward(c, segk, segq, q, kv, left, right):
    q_spec, o_spec, k_spec, v_spec, lse_spec = pair_specs(c)
    return pl.pallas_call(
        attn_fwd_kernel,
        grid=(PAIRS, TOK // QB),
        in_specs=[whole(segk.shape), whole(segq.shape), q_spec] + [k_spec] * 3 + [v_spec] * 3,
        out_specs=[o_spec, lse_spec],
        out_shape=[sds((TOK, HF), BF16), sds((PAIRS, TOK // QB, 1, 2 * QB), F32)],
        scratch_shapes=[
            pltpu.VMEM((3 * TOK, TILE), BF16),
            pltpu.VMEM((TILE, 3 * TOK), BF16),
            pltpu.VMEM((TOK // QB, KSPAN, QB), F32),
        ],
        compiler_params=params(),
        cost_estimate=cost(8e9, 4e6),
        name="attn_fwd",
    )(segk, segq, q, left, kv, right, left, kv, right)


def attn_bwd_kernel(
    segk_ref, segq_ref, q_ref, g_ref, lse_ref, kl, ko, kr, vl, vo, vr,
    dq_ref, dl_ref, do_ref, dr_ref, kext, vext, kturn, bias, dk, dv,
):
    h = pl.program_id(0)
    b = pl.program_id(1)

    @pl.when(b == 0)
    def _():
        fill_keys(kext, kl, ko, kr)
        fill_keys(vext, vl, vo, vr)
        for place, part in enumerate((kl, ko, kr)):
            kturn[:, place * TOK : (place + 1) * TOK] = part[0].T
        dk[...] = jnp.zeros_like(dk)
        dv[...] = jnp.zeros_like(dv)

    @pl.when(h == 0)
    def _():
        fill_bias(bias, segk_ref, segq_ref, b)

    off = pl.multiple_of(b * QB, QB)
    span = pl.ds(off, KSPAN)
    qz = split_pair(q_ref[0])
    gz = split_pair(g_ref[0])
    scores = dot_bt(kext[span, :], qz)
    extra = bias[b]
    weights = jnp.exp(scores + jnp.concatenate((extra, extra), 1) - lse_ref[0, 0])
    d_weights = dot_bt(vext[span, :], gz)
    row_dot = jnp.sum(weights * d_weights, 0, keepdims=True)
    d_scores = (weights * (d_weights - row_dot)).astype(BF16)
    dv[span, :] += dot(weights.astype(BF16), gz)
    dk[span, :] += dot(d_scores, qz)
    turned = dot(kturn[:, span], d_scores)
    dq_ref[...] = (join_pair(turned).T * DH ** (-0.5)).astype(BF16)

    @pl.when(b == TOK // QB - 1)
    def _():
        for which, grads in enumerate((dk, dv)):
            dl_ref[which] = grads[0:TOK].astype(BF16)
            do_ref[which] = grads[TOK : 2 * TOK]
            dr_ref[which] = grads[2 * TOK :].astype(BF16)


def attn_backward(c, segk, segq, q, g, lse, kv, left, right):
    q_spec, o_spec, k_spec, v_spec, lse_spec = pair_specs(c)
    d_spec = pl.BlockSpec((2, TOK, TILE), lambda h, b: (0, 0, h))
    d_shape = (2, TOK, HF)
    return pl.pallas_call(
        attn_bwd_kernel,
        grid=(PAIRS, TOK // QB),
        in_specs=[whole(segk.shape), whole(segq.shape), q_spec, q_spec, lse_spec]
        + [k_spec] * 3
        + [v_spec] * 3,
        out_specs=[o_spec, d_spec, d_spec, d_spec],
        out_shape=[
            sds((TOK, HF), BF16), sds(d_shape, BF16), sds(d_shape, F32), sds(d_shape, BF16),
        ],
        scratch_shapes=[
            pltpu.VMEM((3 * TOK, TILE), BF16),
            pltpu.VMEM((3 * TOK, TILE), BF16),
            pltpu.VMEM((TILE, 3 * TOK), BF16),
            pltpu.VMEM((TOK // QB, KSPAN, QB), F32),
            pltpu.VMEM((3 * TOK, TILE), F32),
            pltpu.VMEM((3 * TOK, TILE), F32),
        ],
        compiler_params=params(),
        cost_estimate=cost(15e9, 8e6),
        name="attn_bwd",
    )(segk, segq, q, g, lse, left, kv, right, left, kv, right)


def feature_sum(near, far):
    return jnp.sum(near, 1, keepdims=True) + jnp.sum(far, 1, keepdims=True)


def norm_pair(near, far):
    mean = feature_sum(near, far) / D
    near = near - mean
    far = far - mean
    inv = lax.rsqrt(feature_sum(near * near, far * far) / D + NORM_EPS)
    return near * inv, far * inv, inv


def norm_pair_back(grads, normed, inv, gains):
    dn = [g * gain for g, gain in zip(grads, gains)]
    first = feature_sum(*dn) / D
    second = feature_sum(*[d * n for d, n in zip(dn, normed)]) / D
    return [inv * (d - first - n * second) for d, n in zip(dn, normed)]


def out_kernel(rc, a0_ref, a1_ref, w00, w01, w10, w11, hid_ref, valid_ref, vec,
               norm_ref, mid_ref, n_ref, inv_ref, stat_ref):
    keep = valid_ref[...]
    first = rc[1] == 0
    a_near = jnp.where(first, a0_ref[...], a1_ref[...])
    a_far = jnp.where(first, a1_ref[...], a0_ref[...])
    resid = []
    sums = []
    for rel_r, (w_near, w_far) in enumerate(((w00, w01), (w10, w11))):
        r = rc[0] ^ rel_r
        branch = (
            dot(a_near, panels(w_near, HF, 0, 3)) + dot(a_far, panels(w_far, HF, 0, 3)) + vec[4 + r]
        )
        total = hid_ref[rel_r].astype(F32) + branch
        resid.append(total)
        sums.append((total * total, branch * branch))

    @pl.when(pl.program_id(0) == 0)
    def _():
        stat_ref[...] = jnp.zeros_like(stat_ref)

    for which in range(2):
        part = (sums[0][which] + sums[1][which]) * keep
        stat_ref[which] += jnp.sum(part, 0, keepdims=True)
    near, far, inv = norm_pair(*resid)
    for rel_r, n in enumerate((near, far)):
        r = rc[0] ^ rel_r
        out = n * vec[8 + r] + vec[10 + r]
        norm_ref[rel_r] = out
        mid_ref[rel_r] = out.astype(BF16)
        n_ref[rel_r] = n
    inv_ref[...] = inv


def out_spec(spot):
    return pl.BlockSpec((3 * HF, TILE), lambda *_: (spot, 0))


def out_forward(rc, attended, pieces, spot, hidden, valid, va):
    rows = 256
    head = pl.BlockSpec((rows, HF), lambda i: (i, 0))
    half = pl.BlockSpec((2, rows, HF), lambda i: (0, i, 0))
    col = pl.BlockSpec((rows, 1), lambda i: (i, 0))
    return pl.pallas_call(
        out_kernel,
        grid=(TOK // rows,),
        in_specs=[SMEM_SPEC, head, head] + [out_spec(spot)] * 4 + [half, col, whole((16, 1, HF))],
        out_specs=[half, half, half, col, whole((2, 1, HF))],
        out_shape=[
            sds((2, TOK, HF), F32), sds((2, TOK, HF), BF16), sds((2, TOK, HF), F32),
            sds((TOK, 1), F32), sds((2, 1, HF), F32),
        ],
        compiler_params=params(),
        cost_estimate=cost(2 * TOK * D * D, 7e6),
        name="attn_out",
    )(rc, *attended, *pieces, hidden, valid, va)


def gelu_parts(u):
    bell = jnp.exp(-0.5 * u * u)
    t = 1.0 / (1.0 + (0.3275911 * 0.7071067811865476) * jnp.abs(u))
    poly = t * (0.5 * 0.254829592 + t * (0.5 * -0.284496736 + t * (
        0.5 * 1.421413741 + t * (0.5 * -1.453152027 + t * (0.5 * 1.061405429)))))
    tail = poly * bell
    below = jnp.where(u >= 0, 1.0 - tail, tail)
    return u * below, below + u * bell * 0.3989422804014327


def ffn_specs(base):
    def spec(rel_c):
        return pl.BlockSpec(
            (STEPS * FT, TILE),
            lambda f: (base + jnp.clip(f - STEPS * rel_c, 0, STEPS - 1), 0),
        )

    return [spec(0), spec(1)] * 2


def up_tile(ref):
    return panels(ref, HF, 0, FT // TILE)


def down_tile(ref):
    return panels(ref, FT, 0, HF // TILE)


def ffn_fwd_kernel(rc, mid_ref, norm_ref, u00, u01, u10, u11, d00, d01, d10, d11, vec, vecu,
                   act_ref, slope_ref, hid_ref, low_ref, n_ref, inv_ref, acc):
    f = pl.program_id(0)

    @pl.when(f == 0)
    def _():
        acc[...] = jnp.zeros_like(acc)

    def step(rel_c, u_near, u_far, d_near, d_far):
        spot = (rc[1] ^ rel_c) * STEPS + f - STEPS * rel_c
        up = dot(mid_ref[0], up_tile(u_near)) + dot(mid_ref[1], up_tile(u_far)) + vecu[spot]
        act, slope = gelu_parts(up)
        act = act.astype(BF16)
        act_ref[...] = act
        slope_ref[...] = slope.astype(BF16)
        acc[0] += dot(act, down_tile(d_near))
        acc[1] += dot(act, down_tile(d_far))

    @pl.when(f < STEPS)
    def _():
        step(0, u00, u10, d00, d10)

    @pl.when(f >= STEPS)
    def _():
        step(1, u01, u11, d01, d11)

    @pl.when(f == 2 * STEPS - 1)
    def _():
        parts = [norm_ref[rel_r] + (acc[rel_r] + vec[6 + (rc[0] ^ rel_r)]) for rel_r in range(2)]
        near, far, inv = norm_pair(*parts)
        for rel_r, n in enumerate((near, far)):
            r = rc[0] ^ rel_r
            out = n * vec[12 + r] + vec[14 + r]
            hid_ref[rel_r] = out
            low_ref[rel_r] = out.astype(BF16)
            n_ref[rel_r] = n
        inv_ref[...] = inv


def ffn_forward(rc, mid, normed, ups, up_base, downs, down_base, va, vb):
    full = whole((2, TOK, HF))
    wide = pl.BlockSpec((TOK, FT), lambda f: (0, f))
    return pl.pallas_call(
        ffn_fwd_kernel,
        grid=(2 * STEPS,),
        in_specs=[SMEM_SPEC, full, full]
        + ffn_specs(up_base)
        + ffn_specs(down_base)
        + [whole(va.shape), whole(vb.shape)],
        out_specs=[wide, wide, full, full, full, whole((TOK, 1))],
        out_shape=[
            sds((TOK, 2 * FFC), BF16), sds((TOK, 2 * FFC), BF16), sds((2, TOK, HF), F32),
            sds((2, TOK, HF), BF16), sds((2, TOK, HF), F32), sds((TOK, 1), F32),
        ],
        scratch_shapes=[pltpu.VMEM((2, TOK, HF), F32)],
        compiler_params=params(),
        cost_estimate=cost(4 * TOK * D * 4 * D, 24e6),
        name="ffn_fwd",
    )(rc, mid, normed, *ups, *downs, va, vb)


def put_tiles(ref, lead, first, block):
    rows, cols = block.shape
    spot = first
    for i in range(rows // TILE):
        for j in range(cols // TILE):
            ref[lead + (spot,)] = block[
                i * TILE : (i + 1) * TILE, j * TILE : (j + 1) * TILE
            ].astype(BF16)
            spot += 1


def ffn_bwd_kernel(rc, g_ref, n2_ref, inv2_ref, mid_ref, act_ref, slope_ref, n1_ref, inv1_ref,
                   u00, u01, u10, u11, d00, d01, d10, d11, vec,
                   gm_ref, gt_ref, dres_ref, dbr_ref, gv_ref, gu_ref, d_two, d_down, d_mid):
    f = pl.program_id(0)
    rs = [rc[0], rc[0] ^ 1]

    def note(which, rel_r, value):
        gv_ref[2 * which + rs[rel_r]] = jnp.sum(value, 0, keepdims=True)

    @pl.when(f == 0)
    def _():
        grads = [g_ref[0], g_ref[1]]
        normed = [n2_ref[0], n2_ref[1]]
        d_resid = norm_pair_back(grads, normed, inv2_ref[...], [vec[12 + r] for r in rs])
        for rel_r in range(2):
            note(4, rel_r, grads[rel_r] * normed[rel_r])
            note(5, rel_r, grads[rel_r])
            d_two[rel_r] = d_resid[rel_r]
            low = d_resid[rel_r].astype(BF16)
            d_down[rel_r] = low
            note(1, rel_r, low.astype(F32))
        d_mid[...] = jnp.zeros_like(d_mid)

    def step(rel_c, u_near, u_far, d_near, d_far):
        spot = (rc[1] ^ rel_c) * STEPS + f - STEPS * rel_c
        d_act = dot_bt(d_down[0], down_tile(d_near)) + dot_bt(d_down[1], down_tile(d_far))
        d_up = (d_act * slope_ref[...].astype(F32)).astype(BF16)
        gu_ref[spot] = jnp.sum(d_up.astype(F32), 0, keepdims=True)
        act = act_ref[...]
        for rel_r, (ref, u_piece) in enumerate(((gm_ref, u_near), (gt_ref, u_far))):
            put_tiles(ref, (0,), 0, dot_at(mid_ref[rel_r], d_up))
            put_tiles(ref, (0,), 12, dot_at(act, d_down[rel_r]))
            d_mid[rel_r] += dot_bt(d_up, up_tile(u_piece))

    @pl.when(f < STEPS)
    def _():
        step(0, u00, u10, d00, d10)

    @pl.when(f >= STEPS)
    def _():
        step(1, u01, u11, d01, d11)

    @pl.when(f == 2 * STEPS - 1)
    def _():
        grads = [d_two[rel_r] + d_mid[rel_r] for rel_r in range(2)]
        normed = [n1_ref[0], n1_ref[1]]
        d_resid = norm_pair_back(grads, normed, inv1_ref[...], [vec[8 + r] for r in rs])
        for rel_r in range(2):
            note(2, rel_r, grads[rel_r] * normed[rel_r])
            note(3, rel_r, grads[rel_r])
            dres_ref[rel_r] = d_resid[rel_r]
            low = d_resid[rel_r].astype(BF16)
            dbr_ref[rel_r] = low
            note(0, rel_r, low.astype(F32))


def ffn_backward(
    rc, g, n2, inv2, mid, act, slope, n1, inv1, ups, up_base, downs, down_base, va
):
    full = whole((2, TOK, HF))
    col = whole((TOK, 1))
    wide = pl.BlockSpec((TOK, FT), lambda f: (0, f))
    tiles = pl.BlockSpec((1, 24, TILE, TILE), lambda f: (f // STEPS, f % STEPS, 0, 0))
    tile_shape = sds((2, 81, TILE, TILE), BF16)
    return pl.pallas_call(
        ffn_bwd_kernel,
        grid=(2 * STEPS,),
        in_specs=[SMEM_SPEC, full, full, col, full, wide, wide, full, col]
        + ffn_specs(up_base)
        + ffn_specs(down_base)
        + [whole(va.shape)],
        out_specs=[tiles, tiles, full, full, whole((12, 1, HF)), whole((2 * STEPS, 1, FT))],
        out_shape=[
            tile_shape, tile_shape, sds((2, TOK, HF), F32), sds((2, TOK, HF), BF16),
            sds((12, 1, HF), F32), sds((2 * STEPS, 1, FT), F32),
        ],
        scratch_shapes=[
            pltpu.VMEM((2, TOK, HF), F32), pltpu.VMEM((2, TOK, HF), BF16),
            pltpu.VMEM((2, TOK, HF), F32),
        ],
        compiler_params=params(),
        cost_estimate=cost(8 * TOK * D * 4 * D, 36e6),
        name="ffn_bwd",
    )(rc, g, n2, inv2, mid, act, slope, n1, inv1, *ups, *downs, va)


def out_bwd_kernel(rc, dbr_ref, a0_ref, a1_ref, w00, w01, w10, w11, gm_in, gt_in,
                   da_ref, gm_ref, gt_ref):
    del gm_in, gt_in
    for rel_c, (w_near, w_far) in enumerate(((w00, w10), (w01, w11))):
        c = rc[1] ^ rel_c
        da_ref[c] = (
            dot_bt(dbr_ref[0], panels(w_near, HF, 0, 3))
            + dot_bt(dbr_ref[1], panels(w_far, HF, 0, 3))
        ).astype(BF16)
        rows = jnp.where(c == 0, a0_ref[...], a1_ref[...])
        put_tiles(gm_ref, (rel_c,), 0, dot_at(rows, dbr_ref[0]))
        put_tiles(gt_ref, (rel_c,), 0, dot_at(rows, dbr_ref[1]))


def out_backward(rc, d_branch, attended, pieces, spot, tiles_m, tiles_t):
    full = whole((2, TOK, HF))
    anywhere = pl.BlockSpec(memory_space=pl.ANY)
    tiles = pl.BlockSpec((2, 9, TILE, TILE), lambda i: (0, 8, 0, 0))
    return pl.pallas_call(
        out_bwd_kernel,
        grid=(1,),
        in_specs=[SMEM_SPEC, full, whole((TOK, HF)), whole((TOK, HF))]
        + [out_spec(spot)] * 4
        + [anywhere, anywhere],
        out_specs=[full, tiles, tiles],
        out_shape=[
            sds((2, TOK, HF), BF16), sds(tiles_m.shape, BF16), sds(tiles_t.shape, BF16),
        ],
        input_output_aliases={8: 1, 9: 2},
        compiler_params=params(),
        cost_estimate=cost(4 * TOK * D * D, 6e6),
        name="out_bwd",
    )(rc, d_branch, *attended, *pieces, tiles_m, tiles_t)


def qkv_bwd_kernel(col, rc, dq_ref, own_ref, left_ref, right_ref, dx_in, x_ref,
                   w00, w01, w10, w11, gm_in, gt_in, dx_ref, gm_ref, gt_ref, gv_ref):
    del gm_in, gt_in
    parts = [dq_ref[...]]
    for which in range(2):
        back = left_ref[which].astype(F32) + right_ref[which].astype(F32)
        parts.append((own_ref[which] + back).astype(BF16))
    gv_ref[0] = jnp.sum(parts[0].astype(F32), 0, keepdims=True)
    gv_ref[1] = jnp.sum(parts[2].astype(F32), 0, keepdims=True)
    for which in range(3):
        put_tiles(gm_ref, (0,), 9 * which, dot_at(x_ref[0], parts[which]))
        put_tiles(gt_ref, (0,), 9 * which, dot_at(x_ref[1], parts[which]))

    def inputs_grad(w_near, w_far):
        for rel_r, w in enumerate((w_near, w_far)):
            total = dx_in[rel_r]
            for which in range(3):
                total += dot_bt(parts[which], panels(w, HF, 3 * which, 3))
            dx_ref[rel_r] = total

    @pl.when(rc[1] == col)
    def _():
        inputs_grad(w00, w10)

    @pl.when(rc[1] != col)
    def _():
        inputs_grad(w01, w11)


def qkv_backward(col, rc, dq, own, left, right, dx, x, pieces, earlier):
    full = pl.BlockSpec((2, TOK, HF), lambda i, s: (0, 0, 0))
    anywhere = pl.BlockSpec(memory_space=pl.ANY)
    tiles = pl.BlockSpec((1, 27, TILE, TILE), lambda i, s: (s[1] ^ col, 0, 0, 0))
    tile_shape = sds((2, 27, TILE, TILE), BF16)
    if earlier is None:
        kernel = lambda rc, *refs: qkv_bwd_kernel(col, rc, *refs[:10], None, None, *refs[10:])
        aliases = {}
        extra = ()
    else:
        kernel = functools.partial(qkv_bwd_kernel, col)
        aliases = {11: 1, 12: 2}
        extra = earlier
    return pl.pallas_call(
        kernel,
        grid_spec=pltpu.PrefetchScalarGridSpec(
            num_scalar_prefetch=1,
            grid=(1,),
            in_specs=[pl.BlockSpec((TOK, HF), lambda i, s: (0, 0)), full, full, full, full, full]
            + [pl.BlockSpec((9 * HF, TILE), lambda i, s: (0, 0))] * 4
            + [anywhere] * len(extra),
            out_specs=[full, tiles, tiles, pl.BlockSpec((2, 1, HF), lambda i, s: (0, 0, 0))],
        ),
        out_shape=[sds((2, TOK, HF), F32), tile_shape, tile_shape, sds((2, 1, HF), F32)],
        input_output_aliases=aliases,
        compiler_params=params(),
        cost_estimate=cost(6 * TOK * D * D, 10e6),
        name="qkv_bwd",
    )(rc, dq, own, left, right, dx, x, *pieces, *extra)


def row_swap(value):
    return lax.ppermute(value, "row", SWAP)


def col_swap(value):
    return lax.ppermute(value, "col", SWAP)


def dp_swap(value, step):
    size = lax.axis_size("dp")
    return lax.ppermute(value, "dp", [(i, i ^ step) for i in range(size)])


def put_panels(ref, spot, block, rows):
    height, width = block.shape
    for i in range(height // rows):
        for j in range(width // TILE):
            ref[spot : spot + rows, :] = block[i * rows : (i + 1) * rows, j * TILE : (j + 1) * TILE]
            spot += rows
    return spot


def pack_kernel(plan, halves, rc, *refs):
    inputs = refs[: len(refs) - len(plan) - len(halves)]
    outs = refs[len(inputs) : len(inputs) + len(plan)]
    for out, entries in zip(outs, plan):
        spot = 0
        for which, rows in entries:
            spot = put_panels(out, spot, inputs[which][0], rows)
    for which, half in zip(halves, refs[len(inputs) + len(plan) :]):
        count = half.shape[0]
        half[...] = outs[which][pl.ds(pl.multiple_of(rc[2] * count, 16), count), :]


def pack(rc, weights, plan, halves):
    specs = []
    for array, layer in weights:
        specs.append(pl.BlockSpec((1,) + array.shape[1:], lambda i, layer=layer: (layer, 0, 0)))
    heights = []
    for entries in plan:
        heights.append(sum(weights[w][0].shape[1] * weights[w][0].shape[2] for w, _ in entries) // TILE)
    shapes = [sds((h, TILE), BF16) for h in heights]
    shapes += [sds((heights[w] // 2, TILE), BF16) for w in halves]
    return pl.pallas_call(
        functools.partial(pack_kernel, plan, halves),
        grid=(1,),
        in_specs=[SMEM_SPEC] + specs,
        out_specs=[whole(shape.shape) for shape in shapes],
        out_shape=shapes,
        compiler_params=params(),
        cost_estimate=cost(1e6, 3 * TILE * 2 * sum(heights)),
        name="pack",
    )(rc, *[array for array, _ in weights])


def tie(value, *others):
    return lax.optimization_barrier((value, others))


class Weights:
    def __init__(self, local, half, after=None):
        self.local = local
        self.near = col_swap(half if after is None else tie(half, *after)[0])

    def relay(self):
        self.far = dp_swap(self.near, 1)

    def pieces(self):
        other = join_by(lax.axis_index("dp") % 2, self.near, self.far)
        return self.local, other, row_swap(self.local), row_swap(other)


LINE_UP = ((0, 2), (2, 1), (1, 3))
LINE_DOWN = ((2, 0), (1, 2), (3, 1))


def send_up(value):
    return lax.ppermute(value, ("row", "col"), LINE_UP)


def send_down(value):
    return lax.ppermute(value, ("row", "col"), LINE_DOWN)


def add_low(*values):
    total = values[0].astype(F32)
    for value in values[1:]:
        total = total + value.astype(F32)
    return total.astype(BF16)


def pick(pair, bit):
    return lax.dynamic_index_in_dim(pair, bit, 0, keepdims=False)


def join_by(bit, near, far):
    return jnp.where(
        bit == 0, jnp.concatenate((near, far), 0), jnp.concatenate((far, near), 0)
    )


def split_rows(value, step, left):
    bit = (lax.axis_index("dp") // step) % 2
    outer = 2 ** left.index(step)
    left.remove(step)
    count, rows = value.shape[:2]
    pair = value.reshape(count, outer, 2, rows // (2 * outer), TILE)
    keep = lax.dynamic_index_in_dim(pair, bit, 2, keepdims=False)
    away = lax.dynamic_index_in_dim(pair, 1 - bit, 2, keepdims=False)
    return keep.reshape(count, rows // 2, TILE), away.reshape(count, rows // 2, TILE)


def stage(value, order, left):
    what = order.pop(0)
    if what == "col":
        count = value.shape[0] // 2
        return value[:count], col_swap(value[count:])
    keep, away = split_rows(value, what, left)
    return keep, dp_swap(away, what)


def reduce_steps(mine, theirs, orders):
    count = mine.shape[1]
    size = lax.axis_size("dp")
    bits = [2**i for i in range(size.bit_length() - 1)]
    got = yield row_swap(theirs)
    bounds = [count * i // len(orders) for i in range(len(orders) + 1)]
    streams = []
    for first, last, order in zip(bounds, bounds[1:], orders):
        value = add_low(mine[:, first:last], got[:, first:last])
        order = [what for what in order if what == "col" or what in bits]
        order += [bit for bit in bits if bit not in order]
        streams.append([value.reshape(-1, TILE, TILE), order, list(bits)])
    while streams[0][1]:
        if len(streams) > 1 and len({tuple(sorted(map(str, s[1]))) for s in streams}) == 1:
            if len(streams[0][1]) < len(bits) + 1:
                lead = 2 if "col" in streams[0][1] else 1
                parts = [s[0].reshape((lead, -1) + s[0].shape[1:]) for s in streams]
                value = jnp.concatenate(parts, 1)
                streams = [[value.reshape((-1,) + value.shape[2:])] + streams[0][1:]]
        sent = [stage(*s) for s in streams]
        got = yield tuple(away for _, away in sent)
        for s, (keep, _), back in zip(streams, sent, got):
            s[0] = add_low(keep, back)
    yield streams[0][0]


class Reduction:
    def __init__(self, mine, theirs, *orders):
        self.steps = reduce_steps(mine, theirs, orders)
        self.left = 2 + lax.axis_size("dp").bit_length() - 1
        self.value = next(self.steps)

    def finish(self):
        while self.left:
            self.value = self.steps.send(self.value)
            self.left -= 1
        return self.value


def advance(value, *reductions):
    live = [red for red in reductions if red.left]
    value, got = tie(value, *[red.value for red in live])
    for red, part in zip(live, got):
        red.value = red.steps.send(part)
        red.left -= 1
    return value


ORDERS = (("x", "col", "z"), ("col", "z", "x"), ("z", "x", "col"))
STREAM = 36
LTILES = 3 * STREAM
DIM_OF = {"col": 0, "x": 1, "z": 2, "w": 3}
STEP_OF = {"x": 1, "z": 2, "w": 4}
MESH = pl.DeviceIdType.MESH


def stream_plan():
    return [[(what, tuple(order[:i])) for i, what in enumerate(order)] for order in
            [order + ("w",) for order in ORDERS]]


def recv_shape(what, settled):
    dims = [2, 2, 2, 2]
    for done in settled + (what,):
        dims[DIM_OF[done]] = 1
    return (dims[0], STREAM, dims[1], dims[2], dims[3], 16, TILE)


def exchange_kernel(spot_ref, vec_ref, m_a1, g_a1, m_b1, g_b1, m_a0, g_a0, m_b0, t_b0,
                    inbox_ref, vsum_ref, buf, extra, vecs, vgot, outbox,
                    load_sem, row_sem, vec_sem, send_sem, recv_sem, out_sem, in_sem, *recv):
    dp = lax.axis_index("dp")
    row = lax.axis_index("row")
    col = lax.axis_index("col")
    bits = {"x": dp % 2, "z": (dp // 2) % 2, "w": (dp // 4) % 2}

    def peer(what):
        if what == "row":
            return {"row": 1 - row}
        if what == "col":
            return {"col": 1 - col}
        step = STEP_OF[what]
        return {"dp": dp + step * (1 - 2 * bits[what])}

    def other(k):
        place = dp
        for what, step in STEP_OF.items():
            if k & step:
                place = place + step * (1 - 2 * bits[what])
        return place

    barrier = pltpu.get_barrier_semaphore()
    for what in ("row", "col"):
        pl.semaphore_signal(barrier, 1, device_id=peer(what), device_id_type=MESH)
    for k in range(1, 8):
        pl.semaphore_signal(barrier, 1, device_id={"dp": other(k)}, device_id_type=MESH)

    loads = []
    for i, (ref, dst) in enumerate((
        (m_a1, buf.at[:, 0:81]), (m_b1, buf.at[:, 81:108]),
        (g_a1, extra.at[:, 0:81]), (g_b1, extra.at[:, 81:108]),
        (m_a0, buf.at[:, 108:189]), (m_b0, buf.at[:, 189:216]), (g_a0, extra.at[:, 108:189]),
    )):
        loads.append(pltpu.make_async_copy(ref, dst, load_sem.at[i]))
        loads[-1].start()
    pl.semaphore_wait(barrier, 9)

    def remote(src, dst, send, got, target):
        return pltpu.make_async_remote_copy(
            src_ref=src, dst_ref=dst, send_sem=send, recv_sem=got, device_id=target,
            device_id_type=MESH,
        )

    row_copy = remote(t_b0, extra.at[:, 189:216], row_sem.at[0], row_sem.at[1], peer("row"))
    row_copy.start()
    vec_order = ("row", "x", "col", "z", "w")
    vec_copies = []
    vecs[0] = vec_ref[...]

    def send_vec(k):
        vec_copies.append(
            remote(vecs.at[k], vgot.at[k], vec_sem.at[0, k], vec_sem.at[1, k], peer(vec_order[k]))
        )
        vec_copies[-1].start()

    def take_vec(k):
        vec_copies[k].wait()
        vecs[k + 1] = vecs[k] + vgot[k]

    send_vec(0)
    plan = stream_plan()

    def region(settled, what, away):
        picks = [slice(None)] * 4
        for done in settled:
            picks[DIM_OF[done]] = pl.ds(0 if done == "col" else bits[done], 1)
        if what is not None:
            if what == "col":
                spot = 1 if away else 0
            else:
                spot = 1 - bits[what] if away else bits[what]
            picks[DIM_OF[what]] = pl.ds(spot, 1)
        return picks

    def spans(picks):
        return [pl.ds(0, 2) if isinstance(p, slice) else p for p in picks]

    copies = {}

    def send(unit, stream, k):
        what, settled = plan[stream][k]
        c, x, z, w = spans(region(settled, what, True))
        tiles = pl.ds(unit * LTILES + stream * STREAM, STREAM)
        index = (unit * 3 + stream) * 4 + k
        copies[index] = remote(
            buf.at[c, tiles, x, z, w], recv[index], send_sem.at[index], recv_sem.at[index],
            peer(what),
        )
        copies[index].start()

    def take(unit, stream, k):
        what, settled = plan[stream][k]
        c, x, z, w = spans(region(settled, what, False))
        index = (unit * 3 + stream) * 4 + k
        copies[index].wait_recv()
        got = recv[index]
        first = unit * LTILES + stream * STREAM

        def one(i, carry):
            tile = pl.ds(first + i, 1)
            buf[c, tile, x, z, w] = buf[c, tile, x, z, w] + got[:, pl.ds(i, 1)]
            return carry

        lax.fori_loop(0, STREAM, one, 0)

    def fold(unit, stream):
        first = unit * LTILES + stream * STREAM

        def one(i, carry):
            buf[:, pl.ds(first + i, 1)] = buf[:, pl.ds(first + i, 1)] + extra[:, pl.ds(first + i, 1)]
            return carry

        lax.fori_loop(0, STREAM, one, 0)

    for unit in range(2):
        for load in loads[4 * unit : 4 * unit + 4]:
            load.wait()
        if unit == 1:
            row_copy.wait()
        for stream in range(3):
            fold(unit, stream)
            send(unit, stream, 0)
    take_vec(0)
    send_vec(1)
    for k in range(4):
        for unit in range(2):
            for stream in range(3):
                take(unit, stream, k)
                if k < 3:
                    send(unit, stream, k + 1)
        take_vec(k + 1)
        if k < 3:
            send_vec(k + 2)
    vsum_ref[...] = vecs[5]

    slots = outbox.shape[1]
    x, z, w = (pl.ds(bits[what], 1) for what in ("x", "z", "w"))

    def fill(k, carry):
        def one(i, inner):
            tile = spot_ref[k * slots + i]
            outbox[pl.ds(k, 1), pl.ds(i, 1)] = buf[0, pl.ds(tile, 1), x, z, w].reshape(
                1, 1, 16, TILE
            )
            return inner

        return lax.fori_loop(0, slots, one, carry)

    lax.fori_loop(0, 8, fill, 0)
    outs = []
    for k in range(1, 8):
        outs.append(
            remote(outbox.at[other(k)], inbox_ref.at[dp], out_sem.at[k], in_sem.at[k],
                   {"dp": other(k)})
        )
        outs[-1].start()
    own = pltpu.make_async_copy(outbox.at[dp], inbox_ref.at[dp], load_sem.at[7])
    own.start()
    own.wait()
    for copy in outs:
        copy.wait()
    for copy in copies.values():
        copy.wait_send()


def exchange(spot, vec, a1, b1, a0, b0, slots):
    def cut(value):
        return value.reshape(value.shape[:2] + (2, 2, 2, 16, TILE))

    anywhere = pl.BlockSpec(memory_space=pl.ANY)
    vmem = pl.BlockSpec(memory_space=pltpu.VMEM)
    recv = []
    for unit in range(2):
        for order in stream_plan():
            recv += [pltpu.VMEM(recv_shape(*step), BF16) for step in order]
    dma = pltpu.SemaphoreType.DMA
    return pl.pallas_call(
        exchange_kernel,
        in_specs=[SMEM_SPEC, vmem] + [anywhere] * 8,
        out_specs=[vmem, vmem],
        out_shape=[sds((8, slots, 16, TILE), BF16), sds(vec.shape, F32)],
        scratch_shapes=[
            pltpu.VMEM((2, 2 * LTILES, 2, 2, 2, 16, TILE), BF16),
            pltpu.VMEM((2, 2 * LTILES, 2, 2, 2, 16, TILE), BF16),
            pltpu.VMEM((6,) + vec.shape, F32),
            pltpu.VMEM((5,) + vec.shape, F32),
            pltpu.VMEM((8, slots, 16, TILE), BF16),
            dma((8,)), dma((2,)), dma((2, 5)), dma((24,)), dma((24,)), dma((8,)), dma((8,)),
        ] + recv,
        compiler_params=pltpu.CompilerParams(
            collective_id=0, has_side_effects=True, vmem_limit_bytes=63 * 1024 * 1024
        ),
        name="exchange",
    )(spot, vec, *map(cut, a1 + b1 + a0 + b0))


def reduce_small(value):
    value = value + row_swap(value)
    value = value + col_swap(value)
    size = lax.axis_size("dp")
    step = 1
    while step < size:
        value = value + lax.ppermute(value, "dp", [(i, i ^ step) for i in range(size)])
        step *= 2
    return value


def tile_places():
    places = []
    for layer in range(LAYERS):
        base = LTILES * (LAYERS - 1 - layer)
        places += [base + 81 + i for i in range(27)]
        places += [base + 72 + i for i in range(9)]
        for rt in range(3):
            for ct in range(12):
                places.append(base + (ct // 4) * 24 + rt * 4 + ct % 4)
        for rt in range(12):
            for ct in range(3):
                places.append(base + (rt // 4) * 24 + 12 + (rt % 4) * 3 + ct)
    return places


def rotate_update(grad_tiles, left_basis, right_basis, old_m, old_v):
    turned = jnp.einsum("...ji,...jk->...ik", left_basis, grad_tiles, precision=HIGHEST)
    rotated = jnp.einsum("...ik,...kl->...il", turned, right_basis, precision=HIGHEST)
    new_m = DECAY * old_m + (1.0 - DECAY) * rotated
    new_v = DECAY * old_v + (1.0 - DECAY) * rotated * rotated
    direction = new_m / (jnp.sqrt(new_v) + ADAM_EPS)
    back_turn = jnp.einsum("...ij,...jk->...ik", left_basis, direction, precision=HIGHEST)
    update = -TILE_RATE * jnp.einsum(
        "...ik,...lk->...il", back_turn, right_basis, precision=HIGHEST
    )
    return (new_m, new_v, update)


def body(
    tokens, cotangent, segments, valid, w_query, w_key, w_value, w_out, w_up, w_down,
    vectors, vector_m, vector_v, tile_order, basis_left, basis_right, tile_m, tile_v,
):
    r = lax.axis_index("row")
    c = lax.axis_index("col")
    rc = jnp.stack((r, c, lax.axis_index("dp") % 2)).astype(jnp.int32)

    def to_tokens(block):
        pair = block[0].reshape(2, TOK, HF)
        return jnp.stack((pick(pair, r), row_swap(pick(pair, 1 - r))), 0)

    def to_block(pair):
        return join_by(r, pair[0], row_swap(pair[1]))[None]

    x = to_tokens(tokens)
    packed, half = pack(
        rc, ((w_query, 0), (w_key, 0), (w_value, 0)), (((0, HF), (1, HF), (2, HF)),), (0,)
    )
    first_w = Weights(packed, half)
    packs = pack(
        rc,
        ((w_up, 0), (w_out, 0), (w_down, 0), (w_query, 1), (w_key, 1), (w_value, 1), (w_out, 1),
         (w_up, 1), (w_down, 1)),
        (
            ((0, HF), (1, HF)),
            ((2, FT),),
            ((3, HF), (4, HF), (5, HF), (6, HF)),
            ((7, HF), (8, FT)),
        ),
        (0, 1, 2, 3),
    )
    first_w.relay()
    up_w = Weights(packs[0], packs[4], (first_w.near,))
    first_pieces = first_w.pieces()
    x, (up_w.near,) = tie(x, up_w.near)
    up_w.relay()
    down_w = Weights(packs[1], packs[5], (up_w.near,))
    qkv_w = [first_pieces, None]
    out_w = [None, None]
    ffn_w = [None, None]

    seg_full = join_by(r, segments[0], row_swap(segments[0]))
    edge = jnp.full((TOK,), -1, jnp.int32)
    seg_ext = lax.dynamic_slice_in_dim(
        jnp.concatenate((edge, seg_full, edge)), (2 * c + r) * TOK, 3 * TOK, 0
    )
    segq = seg_ext[TOK : 2 * TOK].reshape(TOK // QB, 1, QB)
    segk = seg_ext.reshape(3 * TOK, 1)
    keep = lax.dynamic_slice_in_dim(valid[0], r * TOK, TOK, 0).astype(F32).reshape(TOK, 1)
    vas = [vectors[layer, : 8 * D].reshape(16, 1, HF) for layer in range(LAYERS)]
    vbs = [vectors[layer, 8 * D :].reshape(2 * STEPS, 1, FT) for layer in range(LAYERS)]

    hidden = x
    kept = []
    stats = None
    for layer in range(LAYERS):
        q, kv0, kv1 = qkv_forward(rc, x, qkv_w[layer], vas[layer])
        halos = [(send_up(kv0), send_down(kv0))]
        if layer == 0:
            kv1_now, (left, right, down_w.near) = tie(kv1, *halos[0], down_w.near)
            halos[0] = (left, right)
            down_w.relay()
            late_w = Weights(packs[2], packs[6], halos[0])
        else:
            kv1_now, _ = tie(kv1, *halos[0])
        halos.append((send_up(kv1_now), send_down(kv1_now)))
        attended = []
        lse = []
        for col, kv in enumerate((kv0, kv1)):
            out, part = attn_forward(col, segk, segq, q, kv, *halos[col])
            attended.append(out)
            lse.append(part)
            if layer == 0 and col == 0:
                q, (out, late_w.near, down_w.far) = tie(q, out, late_w.near, down_w.far)
                attended[0] = out
                late_w.relay()
                last_w = Weights(packs[3], packs[7], (late_w.near,))
        if layer == 0:
            up_pieces = up_w.pieces()
            down_pieces = down_w.pieces()
            out_w[0] = (up_pieces, 4)
            ffn_w[0] = (up_pieces, 0, down_pieces, 0)
            late_pieces = late_w.pieces()
            qkv_w[1] = late_pieces
            out_w[1] = (late_pieces, 3)
        normed, mid, n1, inv1, stat = out_forward(
            rc, attended, *out_w[layer], hidden, keep, vas[layer]
        )
        if layer == 0:
            stats = stat
            mid, (last_w.near,) = tie(mid, last_w.near)
            last_w.relay()
            last_pieces = last_w.pieces()
            ffn_w[1] = (last_pieces, 0, last_pieces, 3)
        act, slope, hidden, x_next, n2, inv2 = ffn_forward(
            rc, mid, normed, *ffn_w[layer], vas[layer], vbs[layer]
        )
        kept.append((x, q, (kv0, kv1), halos, attended, lse, mid, n1, inv1, act, slope, n2, inv2))
        x = x_next
    final_out = to_block(x)

    grad = to_tokens(cotangent).astype(F32) * keep[None]
    vec_grads = [None] * LAYERS
    layer_tiles = [None] * LAYERS
    for layer in reversed(range(LAYERS)):
        x, q, kvs, halos, attended, lse, mid, n1, inv1, act, slope, n2, inv2 = kept[layer]
        last = layer == 0
        ffn_m, ffn_t, grad, d_branch, gv_mid, gv_up = ffn_backward(
            rc, grad, n2, inv2, mid, act, slope, n1, inv1, *ffn_w[layer], vas[layer]
        )
        d_att, ffn_m, ffn_t = out_backward(
            rc, d_branch, attended, *out_w[layer], ffn_m, ffn_t
        )
        parts = []
        for col in range(2):
            dq, d_left, d_own, d_right = attn_backward(
                col, segk, segq, q, d_att, lse[col], kvs[col], *halos[col]
            )
            parts.append((dq, d_own, send_up(d_right), send_down(d_left)))
            if col == 0:
                d_att, _ = tie(d_att, dq)
        earlier = None
        gv_qkv = []
        for col in range(2):
            grad, qkv_m, qkv_t, gv = qkv_backward(
                col, rc, *parts[col], grad, x, qkv_w[layer], earlier
            )
            earlier = (qkv_m, qkv_t)
            gv_qkv.append(gv)
        layer_tiles[layer] = ((ffn_m, ffn_t), (qkv_m, qkv_t))
        vec_grads[layer] = jnp.concatenate(
            (jnp.stack(gv_qkv, 1).reshape(-1), gv_mid.reshape(-1), gv_up.reshape(-1))
        )
    grad_tokens = to_block(grad)

    vec_len = vectors.shape[1]
    extra = jnp.stack((jnp.sum(stats[0]), jnp.sum(stats[1]), jnp.sum(keep)))
    sums = jnp.concatenate((*vec_grads, extra, jnp.zeros((1021,), F32)))

    owner_code = tile_order[0, 0]
    slots = tile_m.shape[2]
    owners = lax.axis_size("dp")
    targets = owner_code % owners * slots + owner_code // owners
    match = targets[None, :] == jnp.arange(owners * slots)[:, None]
    places = jnp.asarray(tile_places(), jnp.int32)
    spot = jnp.sum(jnp.where(match, places[None, :], 0), 1)
    taken = lax.dynamic_slice_in_dim(
        jnp.any(match, 1), lax.axis_index("dp") * slots, slots, 0
    )
    (ffn0, qkv0), (ffn1, qkv1) = layer_tiles
    if owners == 8:
        inbox, sums = exchange(
            spot,
            sums.reshape(-1, TILE),
            (ffn1[0], row_swap(ffn1[1])),
            (qkv1[0], row_swap(qkv1[1])),
            (ffn0[0], row_swap(ffn0[1])),
            qkv0,
            slots,
        )
        sums = sums.reshape(-1)
    else:
        sums = reduce_small(sums)
        all_tiles = jnp.concatenate(
            [Reduction(*pair, (1, 2, "col")).finish() for pair in (ffn1, qkv1, ffn0, qkv0)], 0
        )
        outbox = jnp.take(all_tiles, spot, axis=0).reshape(owners, slots, TILE // owners, TILE)
        inbox = lax.all_to_all(outbox, "dp", 0, 0, tiled=True)
    vector_grad = sums[: LAYERS * vec_len].reshape(LAYERS, vec_len)
    totals = sums[LAYERS * vec_len : LAYERS * vec_len + 3]
    statistics = jnp.sqrt(totals[:2] / (D * totals[2]))
    bits = owners.bit_length() - 1
    inbox = inbox.reshape((2,) * bits + (slots, TILE // owners, TILE))
    order = (bits,) + tuple(range(bits - 1, -1, -1)) + (bits + 1, bits + 2)
    tile_grad = inbox.transpose(order).reshape(slots, TILE, TILE).astype(F32)
    tile_grad = jnp.where(taken[:, None, None], tile_grad, 0.0)

    vector_m_new = DECAY * vector_m + (1.0 - DECAY) * vector_grad
    vector_v_new = DECAY * vector_v + (1.0 - DECAY) * vector_grad * vector_grad
    vector_update = -VECTOR_RATE * vector_m_new / (jnp.sqrt(vector_v_new) + ADAM_EPS)
    tile_m_new, tile_v_new, tile_update = rotate_update(
        tile_grad, basis_left[0, 0], basis_right[0, 0], tile_m[0, 0], tile_v[0, 0]
    )
    return (
        final_out,
        grad_tokens,
        statistics,
        vector_grad,
        vector_m_new,
        vector_v_new,
        vector_update,
        tile_grad[None, None],
        tile_m_new[None, None],
        tile_v_new[None, None],
        tile_update[None, None],
    )


def solution(mesh):
    weight_rc = P(None, "row", "col")
    weight_cr = P(None, "col", "row")
    slot = P("row", "col", "dp", None, None)
    block = P("dp", "col", "row")
    in_specs = (
        block, block, P("dp", "row"), P("dp", "col"),
        weight_rc, weight_rc, weight_rc, weight_cr, weight_rc, weight_cr,
        P(), P(), P(), P("row", "col", None), slot, slot, slot, slot,
    )
    out_specs = (block, block, P(), P(), P(), P(), P(), slot, slot, slot, slot)
    return jax.shard_map(body, mesh=mesh, in_specs=in_specs, out_specs=out_specs, check_vma=False)
```
